256 devices in a mesh: temp: 64 (over y, z, core), mp: 4 (over x).
Axes of the slice: x: 4, y: 4, z: 8, core: 2. Of those that a mesh axis runs over, the one named last changes fastest.
Arguments:
- chains: bfloat16 [16384, 4096], P('temp', 'mp'), may hold values from 0 to 1
- weights: bfloat16 [4096, 4096], P('temp', 'mp'), may hold values from -0.375 to 0.375
- visible_bias: float32 [4096], replicated, may hold values from -6 to 6
- hidden_bias: float32 [4096], P('mp'), may hold values from -6 to 6
- inv_temps: float32 [64], P('temp'), may hold values from 0.25 to 1
- hidden_thresholds: int32 [2, 16384, 4096], P(None, 'temp', 'mp'), may hold values from 0 to 255
- visible_thresholds: int32 [2, 16384, 4096], P(None, 'temp'), may hold values from 0 to 255
- swap_phase: int32 [256], replicated, may hold values from 0 to 1
- swap_accept: int32 [16384], P('temp'), may hold values 0 or 1
Outputs:
- visible_out: bfloat16 [16384, 4096], P('temp', 'mp')
- hidden_out: bfloat16 [16384, 4096], P('temp', 'mp')
- energy: float32 [16384], P('temp')
The draws below stay inside these ranges and needn't reach their ends.
Inputs may be any that keep to these rules, and one draw needn't show every extreme that they name: `swap_accept`: only entries r * 256 + c with r a lower partner of chain index c are read.
All inputs are finite; a program needn't handle non-finite values. No bound on the sum of `swap_accept` on one device may be relied on, other than what follows from the above.
Results may differ from the reference program's by a relative error of at most 0.0055.
Values may be sent and summed in bfloat16 or wider, within the bound.
A program may use at most 128 MiB of HBM per device.

```python
import math
import jax
import jax.numpy as jnp
from jax import lax

NV = 4096
NH = 4096
CH = 256
SWEEPS = 2
REPLICAS = 64
N_MP = 4


def touch_ends(array, key, smallest, high):
    place = [jax.random.randint(jax.random.fold_in(key, axis), (), 0, length) for axis, length in enumerate(array.shape)]
    main_axis = array.shape.index(max(array.shape))
    neighbour = place[:main_axis] + [(place[main_axis] + 1) % array.shape[main_axis]] + place[main_axis + 1:]
    return array.at[tuple(place)].set(smallest).at[tuple(neighbour)].set(high)


def levels(own_key, dims, pieces, least, largest):
    factor_of = 1.0
    for dim, blocks in pieces:
        heights = jax.random.uniform(jax.random.fold_in(jax.random.fold_in(own_key, 6), dim), (blocks,), jnp.float32, least / len(pieces), largest / len(pieces))
        factor_of = factor_of * jnp.repeat(jnp.exp(heights), dims[dim] // blocks).reshape((-1,) + (1,) * (len(dims) - 1 - dim))
    return factor_of


def gaussian(stream_key, shape, spread, limit, split=(), kind=jnp.bfloat16):
    factor_of = levels(stream_key, shape, split, -0.22, 0.18) if split else 1.0
    array = jax.random.normal(stream_key, shape, jnp.float32) * spread * factor_of
    return jnp.minimum(jnp.maximum(array, -limit), limit).astype(kind)


def setup_inputs(seed: int = 0) -> dict:
    streams_of = jax.random.split(jax.random.key(seed), 10)
    chains = jnp.clip(1.0 * jax.random.uniform(streams_of[0], (REPLICAS * CH, NV), jnp.float32) ** levels(streams_of[0], (REPLICAS * CH, NV), ((0, 64), (1, 4)), -0.2, 0.2), 0.0, 1.0).astype(jnp.bfloat16)
    weights = gaussian(streams_of[1], (NV, NH), (NV // 16) ** -0.5, 0.375, ((0, 64), (1, 4)))
    visible_bias = gaussian(streams_of[2], (NV,), 1.0, 6.0, (), jnp.float32)
    hidden_bias = gaussian(streams_of[3], (NH,), 1.0, 6.0, ((0, 4),), jnp.float32)
    inv_temps = jnp.clip(jnp.exp(math.log(1.0) - 1.3862944 * jax.random.uniform(streams_of[4], (REPLICAS,), jnp.float32) ** levels(streams_of[4], (REPLICAS,), ((0, 64),), -0.2, 0.2)), 0.25, 1.0)
    hidden_thresholds = touch_ends(jax.random.randint(streams_of[5], (SWEEPS, REPLICAS * CH, NH), 0, 256), jax.random.fold_in(streams_of[5], 1), 0, 255).astype(jnp.int32)
    visible_thresholds = touch_ends(jax.random.randint(streams_of[6], (SWEEPS, REPLICAS * CH, NV), 0, 256), jax.random.fold_in(streams_of[6], 1), 0, 255).astype(jnp.int32)
    swap_phase = touch_ends(jax.random.randint(streams_of[7], (CH,), 0, 2), jax.random.fold_in(streams_of[7], 1), 0, 1).astype(jnp.int32)
    swap_accept = touch_ends((jax.random.randint(streams_of[8], (REPLICAS * CH,), 0, 2) < 1).astype(jnp.int32), jax.random.fold_in(streams_of[8], 1), 0, 1)
    return {"chains": chains, "weights": weights, "visible_bias": visible_bias, "hidden_bias": hidden_bias, "inv_temps": inv_temps, "hidden_thresholds": hidden_thresholds, "visible_thresholds": visible_thresholds, "swap_phase": swap_phase, "swap_accept": swap_accept}


def logistic(thresholds):
    level = (thresholds.astype(jnp.float32) + 0.5) / 256.0
    return jnp.log(level) - jnp.log1p(-level)


def sweeps_one(visible, beta_one, hid_thr, vis_thr, weights, visible_bias, hidden_bias):
    group_width = NH // N_MP
    hidden = None
    for sweep in range(SWEEPS):
        hidden_pre = jnp.dot(visible, weights, preferred_element_type=jnp.float32)
        hidden = jax.nn.sigmoid(beta_one * (hidden_pre + hidden_bias) + logistic(hid_thr[sweep])).astype(jnp.bfloat16)
        visible_pre = jnp.zeros((visible.shape[0], NV), jnp.float32)
        for group in range(N_MP):
            part_sum = jnp.dot(hidden[:, group * group_width:(group + 1) * group_width],
                               weights[:, group * group_width:(group + 1) * group_width].T,
                               preferred_element_type=jnp.float32)
            rounded = lax.optimization_barrier(part_sum.astype(jnp.bfloat16))
            visible_pre = visible_pre + rounded.astype(jnp.float32)
        visible = jax.nn.sigmoid(beta_one * (visible_pre + visible_bias) + logistic(vis_thr[sweep])).astype(jnp.bfloat16)
    return visible, hidden


def reference(chains, weights, visible_bias, hidden_bias, inv_temps, hidden_thresholds, visible_thresholds, swap_phase, swap_accept):
    total = inv_temps.shape[0]
    vis_all = chains.reshape(total, CH, NV)
    hid_thr = jnp.transpose(hidden_thresholds.reshape(SWEEPS, total, CH, NH), (1, 0, 2, 3))
    vis_thr = jnp.transpose(visible_thresholds.reshape(SWEEPS, total, CH, NV), (1, 0, 2, 3))

    def one(items):
        return sweeps_one(items[0], items[1], items[2], items[3], weights, visible_bias, hidden_bias)

    vis_new, hid_new = lax.map(one, (vis_all, inv_temps, hid_thr, vis_thr))
    accept = swap_accept.reshape(total, CH)
    parity = swap_phase[None, :]
    replica = jnp.arange(total, dtype=jnp.int32)[:, None]
    is_lower = ((replica % 2) == parity) & (replica + 1 < total)
    is_upper = (((replica - 1) % 2) == parity) & (replica >= 1)
    acc_low = jnp.concatenate([jnp.zeros((1, CH), jnp.int32), accept[:-1]], axis=0)
    take_up = is_lower & (accept == 1)
    take_low = is_upper & (acc_low == 1)

    def moved(states):
        zero_row = jnp.zeros_like(states[:1])
        from_low = jnp.concatenate([zero_row, states[:-1]], axis=0)
        from_up = jnp.concatenate([states[1:], zero_row], axis=0)
        return jnp.where(take_up[:, :, None], from_up, jnp.where(take_low[:, :, None], from_low, states))

    vis_out = moved(vis_new)
    hid_out = moved(hid_new)

    def free_energy(items):
        visible, beta_one = items
        hidden_pre = jnp.dot(visible, weights, preferred_element_type=jnp.float32) + hidden_bias
        soft_sum = jnp.sum(jax.nn.softplus(beta_one * hidden_pre), axis=1)
        bias_sum = jnp.sum(visible.astype(jnp.float32) * visible_bias, axis=1)
        return -(beta_one * bias_sum + soft_sum) / NH

    energy = lax.map(free_energy, (vis_out, inv_temps))
    return vis_out.reshape(total * CH, NV), hid_out.reshape(total * CH, NH), energy.reshape(total * CH)
```

```python
import heapq

import jax
import jax.numpy as jnp
from jax import lax
from jax.experimental import pallas as pl
from jax.experimental.pallas import tpu as pltpu
from jax.sharding import PartitionSpec as P

NH = 4096
SWEEPS = 2
NY, NZ, NX, NT = 4, 8, 4, 64
ROWS, BLK, CW = 256, 1024, 256
F32, BF16 = jnp.float32, jnp.bfloat16
MESH = pl.DeviceIdType.MESH


def gather_plan():
    msgs = []
    for s in (1, -1):
        for d in range(1, 5):
            first, rows = (32, 32) if d < 4 else ((32, 16) if s > 0 else (48, 16))
            msgs.append((("BZ", s, d), (0, 0, s), (0, 0, -s * (d - 1)), first, rows, [("BZ", s, d - 1)] if d > 1 else []))
    msgs.append((("AY", 1, 1), (0, 1, 0), (0, 0, 0), 0, 32, []))
    msgs.append((("AY", -1, 1), (0, -1, 0), (0, 0, 0), 0, 32, []))
    msgs.append((("AY", 1, 2), (0, 1, 0), (0, -1, 0), 0, 16, [("AY", 1, 1)]))
    msgs.append((("AY", -1, 2), (0, -1, 0), (0, 1, 0), 16, 16, [("AY", -1, 1)]))
    there = ([], [("AY", 1, 1)], [("AY", -1, 1)], [("AY", 1, 2), ("AY", -1, 2)])
    for d in range(1, 5):
        for j, oy in enumerate((0, -1, 1, 2)):
            for s in (1, -1):
                if d == 4 and (j < 2) != (s > 0):
                    continue
                deps = there[j] if d == 1 else [("AZ", s, d - 1, j)]
                msgs.append((("AZ", s, d, j), (0, 0, s), (0, oy, -s * (d - 1)), 0, 32, deps))
    for zz in (0, -1, 1, -2, 2, -3, 3, 4):
        deps = [] if zz == 0 else ([("BZ", 1, 4), ("BZ", -1, 4)] if zz == 4 else [("BZ", -1 if zz > 0 else 1, abs(zz))])
        for s in (1, -1):
            msgs.append((("BY", s, 1, zz), (0, s, 0), (0, 0, zz), 32, 32, deps))
        s = 1 if zz in (0, 1, -2, 3) else -1
        msgs.append((("BY", s, 2, zz), (0, s, 0), (0, -s, zz), 32, 32, [("BY", s, 1, zz)]))
    for s in (1, -1):
        for j in (0, 2, 1, 3):
            msgs.append((("AX", s, 1, j), (s, 0, 0), (0, 0, 0), j, 4, []))
        for j in ((0, 1) if s > 0 else (2, 3)):
            msgs.append((("AX", s, 2, j), (s, 0, 0), (-s, 0, 0), j, 4, [("AX", s, 1, j)]))
    return msgs


def arrival_order(msgs):
    free, done, left = {}, set(), {m[0]: m for m in msgs}
    order, events, first = [], [], []

    def issue(now):
        for name in [n for n, m in left.items() if all(d in done for d in m[5])]:
            m = left.pop(name)
            cost = m[4] / 32 * (1.4 if m[1][0] == 0 else 0.7 * 32 / 4 * 4 / 8)
            begin = max(now, free.get(m[1], 0.0))
            free[m[1]] = begin + cost
            heapq.heappush(events, (begin + cost + 2.0, len(order), name))
            order.append((name, now))

    issue(0.0)
    sends = {None: [n for n, _ in order]}
    waits = []
    while events:
        now, _, name = heapq.heappop(events)
        done.add(name)
        waits.append(name)
        before = len(order)
        issue(now)
        sends[name] = [n for n, _ in order[before:]]
    return sends, waits


MSGS = gather_plan()
INDEX = {m[0]: i for i, m in enumerate(MSGS)}
SENDS, WAITS = arrival_order(MSGS)


def kernel(
    chains, weights, vbias, hbias, temps, hthr, vthr, phase, accept,
    vis_out, hid_out, energy_out,
    W, V, thr, L, acc, H, SB, RB, PF, meta, metar, swapv, swaph, vo, ho, BT, TU, TL, ebuf,
    gs, gr, dsem, ags, agr, rss, rsr, sws, swr, ms, mr, es, er, lsem,
):
    t = lax.axis_index("temp")
    m = lax.axis_index("mp")
    c = lax.rem(t, 2)
    z = lax.rem(t // 2, NZ)
    y = t // (2 * NZ)

    def col(d):
        return lax.rem(m + d + NX, NX)

    def rep(d):
        return lax.rem(t + d + NT, NT)

    def temp_of(dy, dz):
        return (lax.rem(y + dy + NY, NY) * NZ + lax.rem(z + dz + NZ, NZ)) * 2 + c

    pending = []

    def send(src, dst, ssem, rsem, device):
        copy = pltpu.make_async_remote_copy(
            src_ref=src, dst_ref=dst, send_sem=ssem, recv_sem=rsem, device_id=device, device_id_type=MESH
        )
        copy.start()
        return copy

    def arrived(ref, sem):
        pltpu.make_async_copy(ref, ref, sem).wait()

    wload = pltpu.make_async_copy(weights, W.at[pl.ds(pl.multiple_of(t * 64, 64), 64)], lsem.at[0])
    wload.start()
    vload = []
    for j in range(4):
        cp = pltpu.make_async_copy(chains.at[:, pl.ds(j * CW, CW)], V.at[0, 4 * m + j], lsem.at[1 + j])
        cp.start()
        vload.append(cp)
    tload = []
    for s in range(SWEEPS):
        cp = pltpu.make_async_copy(hthr.at[s], thr.at[2 * s], lsem.at[5 + 2 * s])
        cp.start()
        tload.append(cp)
        cp = pltpu.make_async_copy(
            vthr.at[s, :, pl.ds(pl.multiple_of(m * BLK, BLK), BLK)], thr.at[2 * s + 1], lsem.at[6 + 2 * s]
        )
        cp.start()
        tload.append(cp)
    beta = temps[0:1, 0:1]
    meta[...] = jnp.broadcast_to(beta, (8, 128))
    meta[0:2, :] = accept[...].astype(F32)

    barrier = pltpu.get_barrier_semaphore()
    peers = [(t, col(d)) for d in (1, 2, 3)]
    peers += [(rep(e), col(d)) for e in (1, -1) for d in range(4)]
    peers += [(temp_of(1, 0), m), (temp_of(-1, 0), m), (temp_of(0, 1), m), (temp_of(0, -1), m)]
    for p in peers:
        pl.semaphore_signal(barrier, inc=1, device_id=p, device_id_type=MESH)
    pl.semaphore_wait(barrier, len(peers))

    sibling = (t + 1 - 2 * c, m)

    def rows_of(oy, oz, first, rows):
        start = temp_of(oy, oz) * 64 + first
        return W.at[pl.ds(pl.multiple_of(start, 16), rows)]

    def place(msg, seen):
        name, (sx, sy, sz), (ox, oy, oz), first, rows, _ = msg
        if sx:
            return V.at[0, 4 * col(ox - (sx if seen else 0)) + first]
        return rows_of(oy - (sy if seen else 0), oz - (sz if seen else 0), first, rows)

    def launch(name):
        msg = MSGS[INDEX[name]]
        sx, sy, sz = msg[1]
        ref = place(msg, False)
        device = (t, col(sx)) if sx else (temp_of(sy, sz), m)
        i = INDEX[name]
        pending.append(send(ref, ref, gs.at[i], gr.at[i], device))

    def to_sibling(ref):
        send(ref, ref, dsem.at[0], dsem.at[1], sibling)

    wload.wait()
    for name in SENDS[None]:
        if name[0] != "AX":
            launch(name)
    to_sibling(W.at[pl.ds(pl.multiple_of(t * 64, 64), 64)])
    for cp in vload:
        cp.wait()
    for name in SENDS[None]:
        if name[0] == "AX":
            launch(name)
    for e in (0, 1):
        pending.append(send(meta, metar.at[e], ms.at[e], mr.at[e], (rep(1 - 2 * e), m)))

    def prepare(k):
        tload[k].wait()

        def some(i, carry):
            r = pl.ds(pl.multiple_of(i * 32, 32), 32)
            level = (thr[k, r, :].astype(F32) + 0.5) / 256.0
            bias = hbias[...] if k % 2 == 0 else vbias[m]
            L[k, r, :] = beta * bias + (jnp.log(level) - jnp.log(1.0 - level))
            return carry

        lax.fori_loop(0, ROWS // 32, some, 0)

    def decisions():
        for e in (0, 1):
            arrived(metar.at[e], mr.at[e])
        low, up = metar.at[0], metar.at[1]
        ph = phase[...]
        lower = (lax.rem(t, 2) == ph) & (t + 1 < NT)
        upper = (lax.rem(t + 1, 2) == ph) & (t >= 1)
        take_up = jnp.where(lower & (accept[...] == 1), 1.0, 0.0)
        take_low = jnp.where(upper & (low[0:2, :] > 0.5), 1.0, 0.0)
        b = jnp.where(take_up > 0.5, up[2:4, :], jnp.where(take_low > 0.5, low[2:4, :], jnp.broadcast_to(beta, (2, 128))))
        for h in (0, 1):
            for ref, rows in ((TU, take_up), (TL, take_low), (BT, b)):
                ref[128 * h : 128 * h + 128, :] = jnp.broadcast_to(rows[h : h + 1, :], (128, 128)).T
        return take_up, take_low

    extra = {4: 0, 8: 1, 12: 2, 16: 3}
    flags = None
    for n, name in enumerate(WAITS):
        msg = MSGS[INDEX[name]]
        ref = place(msg, True)
        arrived(ref, gr.at[INDEX[name]])
        for nxt in SENDS[name]:
            launch(nxt)
        if name[0] != "AX":
            to_sibling(ref)
        if n in extra:
            prepare(extra[n])
        if n == 20:
            flags = decisions()
    take_up, take_low = flags
    half = W.at[pl.ds(0, NT // 2 * 64)]
    arrived(half, dsem.at[1])

    def dot(a, b):
        return jnp.dot(a, b, preferred_element_type=F32)

    def wtile(b, j, n, width):
        return W[pl.ds(pl.multiple_of(b * BLK + j * CW, CW), CW), pl.ds(pl.multiple_of(n * width, width), width)]

    def add_product(a, blocks, fresh):
        def tile(n, carry):
            cols = pl.ds(pl.multiple_of(n * 256, 256), 256)
            total = None
            for b, j in blocks:
                part = dot(V[a, 4 * b + j], wtile(b, j, n, 256))
                total = part if total is None else total + part
            acc[:, cols] = total if fresh else acc[:, cols] + total
            return carry

        lax.fori_loop(0, 4, tile, 0)

    def gathered_product(a):
        add_product(a, [(m, j) for j in range(4)], True)
        for j in (0, 2, 1, 3):
            arrived(V.at[a, 4 * col(-1) + j], agr.at[a - 1, j])
            if j < 2:
                ref = V.at[a, 4 * col(-1) + j]
                pending.append(send(ref, ref, ags.at[a - 1, 4 + j], agr.at[a - 1, 4 + j], (t, col(1))))
            arrived(V.at[a, 4 * col(1) + j], agr.at[a - 1, 6 + j])
            if j >= 2:
                ref = V.at[a, 4 * col(1) + j]
                pending.append(send(ref, ref, ags.at[a - 1, 8 + j], agr.at[a - 1, 8 + j], (t, col(-1))))
            add_product(a, [(col(-1), j), (col(1), j)], False)
        for f in (0, 1):
            arrived(V.at[a, 4 * col(2) + f], agr.at[a - 1, 4 + f])
            arrived(V.at[a, 4 * col(2) + 2 + f], agr.at[a - 1, 10 + f])
            add_product(a, [(col(2), f), (col(2), 2 + f)], False)

    def hidden_states(s):
        def tile(n, carry):
            cols = pl.ds(pl.multiple_of(n * 256, 256), 256)
            H[s, :, cols] = jax.nn.sigmoid(beta * acc[:, cols] + L[2 * s, :, cols]).astype(BF16)
            return carry

        lax.fori_loop(0, 4, tile, 0)

    def partial(s, b, j):
        return lax.dot_general(
            H[s], W[pl.ds(pl.multiple_of(b * BLK + j * CW, CW), CW), :], (((1,), (1,)), ((), ())),
            preferred_element_type=F32,
        )

    def order(i):
        return lax.rem(2 * i, 4) + lax.rem(i, 4) // 2

    def visible_states(s):
        def first(i, carry):
            g, j = i // 4, order(i)
            sg = 1 - 2 * (j // 2)
            b = jnp.where(g == 0, col(2), col(-sg))
            target = jnp.where(g == 0, col(sg), col(-sg))
            k = 4 * g + j
            SB[s, k] = partial(s, b, j).astype(BF16)
            send(SB.at[s, k], RB.at[s, k], rss.at[s, k], rsr.at[s, k], (t, target))
            return carry

        lax.fori_loop(0, 8, first, 0)

        def merge(i, carry):
            j = order(i)
            sg = 1 - 2 * (j // 2)
            term = partial(s, col(sg), j)
            arrived(RB.at[s, j], rsr.at[s, j])
            SB[s, 8 + j] = (term + RB[s, j].astype(F32)).astype(BF16)
            send(SB.at[s, 8 + j], RB.at[s, 8 + j], rss.at[s, 8 + j], rsr.at[s, 8 + j], (t, col(sg)))
            return carry

        lax.fori_loop(0, 4, merge, 0)

        def own(j, carry):
            PF[j] = partial(s, m, j)
            return carry

        lax.fori_loop(0, 4, own, 0)

        def last(i, carry):
            j = order(i)
            arrived(RB.at[s, 4 + j], rsr.at[s, 4 + j])
            arrived(RB.at[s, 8 + j], rsr.at[s, 8 + j])
            pre = PF[j] + RB[s, 4 + j].astype(F32) + RB[s, 8 + j].astype(F32)
            cols = pl.ds(pl.multiple_of(j * CW, CW), CW)
            V[s + 1, 4 * m + j] = jax.nn.sigmoid(beta * pre + L[2 * s + 1, :, cols]).astype(BF16)
            ref = V.at[s + 1, 4 * m + j]
            send(ref, ref, ags.at[s, j], agr.at[s, j], (t, col(1)))
            send(ref, ref, ags.at[s, 6 + j], agr.at[s, 6 + j], (t, col(-1)))
            return carry

        lax.fori_loop(0, 4, last, 0)

    add_product(0, [(b, j) for b in range(4) for j in range(4)], True)
    hidden_states(0)
    visible_states(0)
    gathered_product(1)
    hidden_states(1)
    for e in (0, 1):
        pending.append(send(H.at[1], swaph.at[e], sws.at[e], swr.at[e], (rep(1 - 2 * e), m)))
    visible_states(1)
    mine = V.at[2, pl.ds(4 * m, 4)]
    for e in (0, 1):
        pending.append(send(mine, swapv.at[e], sws.at[2 + e], swr.at[2 + e], (rep(1 - 2 * e), m)))

    gathered_product(2)

    def bias_part(g, total):
        return total + V[2, 4 * m + g // 2, :, pl.ds(pl.multiple_of(lax.rem(g, 2) * 128, 128), 128)].astype(F32) * vbias[
            m, :, pl.ds(pl.multiple_of(g * 128, 128), 128)
        ]

    total = BT[...] * lax.fori_loop(0, 8, bias_part, jnp.zeros((ROWS, 128), F32))

    def soft_part(g, total):
        cols = pl.ds(pl.multiple_of(g * 128, 128), 128)
        x = BT[...] * (acc[:, cols] + hbias[:, cols])
        return total + (jnp.maximum(x, 0.0) + jnp.log1p(jnp.exp(-jnp.abs(x))))

    total = lax.fori_loop(0, 8, soft_part, total)
    ebuf[0, m] = jnp.zeros((8, 128), F32)
    for h in (0, 1):
        ebuf[0, m, h : h + 1, :] = jnp.sum(total[128 * h : 128 * h + 128, :].T, axis=0, keepdims=True) * (-1.0 / NH)
    targets = [(0, d) for d in (1, 2, 3)] + [(e, d) for e in (1, -1) for d in range(4)]
    for e, d in targets:
        i = (e % 3) * 4 + d
        pending.append(send(ebuf.at[0, m], ebuf.at[e % 3, m], es.at[i], er.at[i], (rep(e), col(d))))

    for e in (0, 1):
        arrived(swaph.at[e], swr.at[e])

    def swap_hidden(g, carry):
        cols = pl.ds(pl.multiple_of(g * 128, 128), 128)
        low, up, own = swaph[0, :, cols].astype(F32), swaph[1, :, cols].astype(F32), H[1, :, cols].astype(F32)
        ho[:, cols] = jnp.where(TU[...] > 0.5, up, jnp.where(TL[...] > 0.5, low, own)).astype(BF16)
        return carry

    lax.fori_loop(0, 8, swap_hidden, 0)
    hput = pltpu.make_async_copy(ho, hid_out, lsem.at[9])
    hput.start()
    for e in (0, 1):
        arrived(swapv.at[e], swr.at[2 + e])

    def swap_visible(g, carry):
        cols = pl.ds(pl.multiple_of(lax.rem(g, 2) * 128, 128), 128)
        k = g // 2
        low, up = swapv[0, k, :, cols].astype(F32), swapv[1, k, :, cols].astype(F32)
        own = V[2, 4 * m + k, :, cols].astype(F32)
        vo[:, pl.ds(pl.multiple_of(g * 128, 128), 128)] = jnp.where(
            TU[...] > 0.5, up, jnp.where(TL[...] > 0.5, low, own)
        ).astype(BF16)
        return carry

    lax.fori_loop(0, 8, swap_visible, 0)
    vput = pltpu.make_async_copy(vo, vis_out, lsem.at[10])
    vput.start()
    for e, d in targets:
        arrived(ebuf.at[e % 3, col(-d)], er.at[(e % 3) * 4 + d])

    def summed(k):
        return ebuf[k, 0, 0:2, :] + ebuf[k, 1, 0:2, :] + ebuf[k, 2, 0:2, :] + ebuf[k, 3, 0:2, :]

    energy_out[...] = jnp.where(take_up > 0.5, summed(2), jnp.where(take_low > 0.5, summed(1), summed(0)))

    for copy in pending:
        copy.wait_send()
    arrived(half, dsem.at[0])
    for s in range(SWEEPS):

        def left(k, carry):
            arrived(SB.at[s, k], rss.at[s, k])
            return carry

        lax.fori_loop(0, 12, left, 0)
        for j in range(4):
            arrived(V.at[s + 1, j], ags.at[s, j])
            arrived(V.at[s + 1, j], ags.at[s, 6 + j])
    hput.wait()
    vput.wait()


def on_device(
    chains, weights, visible_bias, hidden_bias, inv_temps, hidden_thresholds, visible_thresholds, swap_phase, swap_accept
):
    vmem = pl.BlockSpec(memory_space=pltpu.VMEM)
    hbm = pl.BlockSpec(memory_space=pl.ANY)
    dma = pltpu.SemaphoreType.DMA
    n = len(MSGS)
    vis, hid, energy = pl.pallas_call(
        kernel,
        out_shape=(
            jax.ShapeDtypeStruct((ROWS, BLK), BF16),
            jax.ShapeDtypeStruct((ROWS, BLK), BF16),
            jax.ShapeDtypeStruct((2, 128), F32),
        ),
        in_specs=[hbm, hbm, vmem, vmem, vmem, hbm, hbm, vmem, vmem],
        out_specs=(hbm, hbm, vmem),
        scratch_shapes=[
            pltpu.VMEM((4096, BLK), BF16),
            pltpu.VMEM((3, 16, ROWS, CW), BF16),
            pltpu.VMEM((4, ROWS, BLK), jnp.int32),
            pltpu.VMEM((4, ROWS, BLK), F32),
            pltpu.VMEM((ROWS, BLK), F32),
            pltpu.VMEM((2, ROWS, BLK), BF16),
            pltpu.VMEM((2, 12, ROWS, CW), BF16),
            pltpu.VMEM((2, 12, ROWS, CW), BF16),
            pltpu.VMEM((4, ROWS, CW), F32),
            pltpu.VMEM((8, 128), F32),
            pltpu.VMEM((2, 8, 128), F32),
            pltpu.VMEM((2, 4, ROWS, CW), BF16),
            pltpu.VMEM((2, ROWS, BLK), BF16),
            pltpu.VMEM((ROWS, BLK), BF16),
            pltpu.VMEM((ROWS, BLK), BF16),
            pltpu.VMEM((ROWS, 128), F32),
            pltpu.VMEM((ROWS, 128), F32),
            pltpu.VMEM((ROWS, 128), F32),
            pltpu.VMEM((3, 4, 8, 128), F32),
            dma((n,)), dma((n,)), dma((2,)),
            dma((2, 12)), dma((2, 12)), dma((2, 12)), dma((2, 12)),
            dma((4,)), dma((4,)), dma((2,)), dma((2,)), dma((12,)), dma((12,)), dma((11,)),
        ],
        compiler_params=pltpu.CompilerParams(
            collective_id=0, has_side_effects=True, vmem_limit_bytes=58 * 2**20
        ),
        name="tempered",
    )(
        chains,
        weights,
        visible_bias.reshape(4, 1, BLK),
        hidden_bias.reshape(1, BLK),
        inv_temps.reshape(1, 1),
        hidden_thresholds,
        visible_thresholds,
        swap_phase.reshape(2, 128),
        swap_accept.reshape(2, 128),
    )
    return vis, hid, energy.reshape(ROWS)


def solution(mesh):
    return jax.shard_map(
        on_device,
        mesh=mesh,
        in_specs=(
            P("temp", "mp"),
            P("temp", "mp"),
            P(),
            P("mp"),
            P("temp"),
            P(None, "temp", "mp"),
            P(None, "temp", None),
            P(),
            P("temp"),
        ),
        out_specs=(P("temp", "mp"), P("temp", "mp"), P("temp")),
        check_vma=False,
    )
```

```python
import heapq

import jax
import jax.numpy as jnp
from jax import lax
from jax.experimental import pallas as pl
from jax.experimental.pallas import tpu as pltpu
from jax.sharding import PartitionSpec as P

NH = 4096
SWEEPS = 2
NY, NZ, NX, NT = 4, 8, 4, 64
ROWS, BLK, CW = 256, 1024, 256
F32, BF16 = jnp.float32, jnp.bfloat16
MESH = pl.DeviceIdType.MESH


def gather_plan():
    msgs = []
    for s in (1, -1):
        for d in range(1, 5):
            first, rows = (32, 32) if d < 4 else ((32, 16) if s > 0 else (48, 16))
            msgs.append((("BZ", s, d), (0, 0, s), (0, 0, -s * (d - 1)), first, rows, [("BZ", s, d - 1)] if d > 1 else []))
    msgs.append((("AY", 1, 1), (0, 1, 0), (0, 0, 0), 0, 32, []))
    msgs.append((("AY", -1, 1), (0, -1, 0), (0, 0, 0), 0, 32, []))
    msgs.append((("AY", 1, 2), (0, 1, 0), (0, -1, 0), 0, 16, [("AY", 1, 1)]))
    msgs.append((("AY", -1, 2), (0, -1, 0), (0, 1, 0), 16, 16, [("AY", -1, 1)]))
    there = ([], [("AY", 1, 1)], [("AY", -1, 1)], [("AY", 1, 2), ("AY", -1, 2)])
    for d in range(1, 5):
        for j, oy in enumerate((0, -1, 1, 2)):
            for s in (1, -1):
                if d == 4 and (j < 2) != (s > 0):
                    continue
                deps = there[j] if d == 1 else [("AZ", s, d - 1, j)]
                msgs.append((("AZ", s, d, j), (0, 0, s), (0, oy, -s * (d - 1)), 0, 32, deps))
    for zz in (0, -1, 1, -2, 2, -3, 3, 4):
        deps = [] if zz == 0 else ([("BZ", 1, 4), ("BZ", -1, 4)] if zz == 4 else [("BZ", -1 if zz > 0 else 1, abs(zz))])
        for s in (1, -1):
            msgs.append((("BY", s, 1, zz), (0, s, 0), (0, 0, zz), 32, 32, deps))
        s = 1 if zz in (0, 1, -2, 3) else -1
        msgs.append((("BY", s, 2, zz), (0, s, 0), (0, -s, zz), 32, 32, [("BY", s, 1, zz)]))
    for s in (1, -1):
        for j in (0, 2, 1, 3):
            msgs.append((("AX", s, 1, j), (s, 0, 0), (0, 0, 0), j, 4, []))
        for j in ((0, 1) if s > 0 else (2, 3)):
            msgs.append((("AX", s, 2, j), (s, 0, 0), (-s, 0, 0), j, 4, [("AX", s, 1, j)]))
    return msgs


def arrival_order(msgs):
    free, done, left = {}, set(), {m[0]: m for m in msgs}
    order, events, first = [], [], []

    def issue(now):
        for name in [n for n, m in left.items() if all(d in done for d in m[5])]:
            m = left.pop(name)
            cost = 2.8 if m[1][0] else 1.4 * m[4] / 32
            begin = max(now, free.get(m[1], 0.0))
            free[m[1]] = begin + cost
            heapq.heappush(events, (begin + cost + 2.0, len(order), name))
            order.append((name, now))

    issue(0.0)
    sends = {None: [n for n, _ in order]}
    waits = []
    while events:
        now, _, name = heapq.heappop(events)
        done.add(name)
        waits.append(name)
        before = len(order)
        issue(now)
        sends[name] = [n for n, _ in order[before:]]
    return sends, waits


MSGS = gather_plan()
INDEX = {m[0]: i for i, m in enumerate(MSGS)}
SENDS, WAITS = arrival_order(MSGS)


def kernel(
    chains, weights, vbias, hbias, temps, hthr, vthr, phase, accept,
    vis_out, hid_out, energy_out,
    W, V, thr, L, acc, H, SB, RB, PF, meta, metar, swapv, swaph, vo, ho, BT, TU, TL, ebuf,
    gs, gr, dsem, ags, agr, rss, rsr, sws, swr, ms, mr, es, er, lsem,
):
    t = lax.axis_index("temp")
    m = lax.axis_index("mp")
    c = lax.rem(t, 2)
    z = lax.rem(t // 2, NZ)
    y = t // (2 * NZ)

    def col(d):
        return lax.rem(m + d + NX, NX)

    def rep(d):
        return lax.rem(t + d + NT, NT)

    def temp_of(dy, dz):
        return (lax.rem(y + dy + NY, NY) * NZ + lax.rem(z + dz + NZ, NZ)) * 2 + c

    pending = []

    def send(src, dst, ssem, rsem, device):
        copy = pltpu.make_async_remote_copy(
            src_ref=src, dst_ref=dst, send_sem=ssem, recv_sem=rsem, device_id=device, device_id_type=MESH
        )
        copy.start()
        return copy

    def arrived(ref, sem):
        pltpu.make_async_copy(ref, ref, sem).wait()

    wload = pltpu.make_async_copy(weights, W.at[pl.ds(pl.multiple_of(t * 64, 64), 64)], lsem.at[0])
    wload.start()
    vload = []
    for j in range(4):
        cp = pltpu.make_async_copy(chains.at[:, pl.ds(j * CW, CW)], V.at[0, 4 * m + j], lsem.at[1 + j])
        cp.start()
        vload.append(cp)
    tload = []
    for s in range(SWEEPS):
        cp = pltpu.make_async_copy(hthr.at[s], thr.at[2 * s], lsem.at[5 + 2 * s])
        cp.start()
        tload.append(cp)
        cp = pltpu.make_async_copy(
            vthr.at[s, :, pl.ds(pl.multiple_of(m * BLK, BLK), BLK)], thr.at[2 * s + 1], lsem.at[6 + 2 * s]
        )
        cp.start()
        tload.append(cp)
    beta = temps[0:1, 0:1]
    meta[...] = jnp.broadcast_to(beta, (8, 128))
    meta[0:2, :] = accept[...].astype(F32)

    barrier = pltpu.get_barrier_semaphore()
    peers = [(t, col(1)), (t, col(-1)), (rep(1), m), (rep(-1), m)]
    peers += [(temp_of(1, 0), m), (temp_of(-1, 0), m), (temp_of(0, 1), m), (temp_of(0, -1), m)]
    for p in peers:
        pl.semaphore_signal(barrier, inc=1, device_id=p, device_id_type=MESH)
    pl.semaphore_wait(barrier, len(peers))

    sibling = (t + 1 - 2 * c, m)

    def rows_of(oy, oz, first, rows):
        start = temp_of(oy, oz) * 64 + first
        return W.at[pl.ds(pl.multiple_of(start, 16), rows)]

    def place(msg, seen):
        name, (sx, sy, sz), (ox, oy, oz), first, rows, _ = msg
        if sx:
            return V.at[0, 4 * col(ox - (sx if seen else 0)) + first]
        return rows_of(oy - (sy if seen else 0), oz - (sz if seen else 0), first, rows)

    def launch(name):
        msg = MSGS[INDEX[name]]
        sx, sy, sz = msg[1]
        ref = place(msg, False)
        device = (t, col(sx)) if sx else (temp_of(sy, sz), m)
        i = INDEX[name]
        pending.append(send(ref, ref, gs.at[i], gr.at[i], device))

    def to_sibling(ref):
        send(ref, ref, dsem.at[0], dsem.at[1], sibling)

    wload.wait()
    for name in SENDS[None]:
        if name[0] != "AX":
            launch(name)
    to_sibling(W.at[pl.ds(pl.multiple_of(t * 64, 64), 64)])
    for cp in vload:
        cp.wait()
    for name in SENDS[None]:
        if name[0] == "AX":
            launch(name)
    for e in (0, 1):
        pending.append(send(meta, metar.at[e], ms.at[e], mr.at[e], (rep(1 - 2 * e), m)))

    def prepare(k):
        tload[k].wait()

        def some(i, carry):
            r = pl.ds(pl.multiple_of(i * 32, 32), 32)
            level = (thr[k, r, :].astype(F32) + 0.5) / 256.0
            bias = hbias[...] if k % 2 == 0 else vbias[m]
            L[k, r, :] = beta * bias + (jnp.log(level) - jnp.log(1.0 - level))
            return carry

        lax.fori_loop(0, ROWS // 32, some, 0)

    def decisions():
        for e in (0, 1):
            arrived(metar.at[e], mr.at[e])
        low, up = metar.at[0], metar.at[1]
        ph = phase[...]
        lower = (lax.rem(t, 2) == ph) & (t + 1 < NT)
        upper = (lax.rem(t + 1, 2) == ph) & (t >= 1)
        take_up = jnp.where(lower & (accept[...] == 1), 1.0, 0.0)
        take_low = jnp.where(upper & (low[0:2, :] > 0.5), 1.0, 0.0)
        b = jnp.where(take_up > 0.5, up[2:4, :], jnp.where(take_low > 0.5, low[2:4, :], jnp.broadcast_to(beta, (2, 128))))
        for h in (0, 1):
            for ref, rows in ((TU, take_up), (TL, take_low), (BT, b)):
                ref[128 * h : 128 * h + 128, :] = jnp.broadcast_to(rows[h : h + 1, :], (128, 128)).T
        return take_up, take_low

    extra = {4: 0, 8: 1, 12: 2, 16: 3}
    flags = None
    for n, name in enumerate(WAITS):
        msg = MSGS[INDEX[name]]
        ref = place(msg, True)
        arrived(ref, gr.at[INDEX[name]])
        for nxt in SENDS[name]:
            launch(nxt)
        if name[0] != "AX":
            to_sibling(ref)
        if n in extra:
            prepare(extra[n])
        if n == 20:
            flags = decisions()
    take_up, take_low = flags
    half = W.at[pl.ds(0, NT // 2 * 64)]
    arrived(half, dsem.at[1])

    def dot(a, b):
        return jnp.dot(a, b, preferred_element_type=F32)

    def wtile(b, j, n, width):
        return W[pl.ds(pl.multiple_of(b * BLK + j * CW, CW), CW), pl.ds(pl.multiple_of(n * width, width), width)]

    def add_product(a, blocks, fresh):
        def tile(n, carry):
            cols = pl.ds(pl.multiple_of(n * 256, 256), 256)
            total = None
            for b, j in blocks:
                part = dot(V[a, 4 * b + j], wtile(b, j, n, 256))
                total = part if total is None else total + part
            acc[:, cols] = total if fresh else acc[:, cols] + total
            return carry

        lax.fori_loop(0, 4, tile, 0)

    def gathered_product(a):
        add_product(a, [(m, j) for j in range(4)], True)
        for j in (0, 2, 1, 3):
            arrived(V.at[a, 4 * col(-1) + j], agr.at[a - 1, j])
            if j < 2:
                ref = V.at[a, 4 * col(-1) + j]
                pending.append(send(ref, ref, ags.at[a - 1, 4 + j], agr.at[a - 1, 4 + j], (t, col(1))))
            arrived(V.at[a, 4 * col(1) + j], agr.at[a - 1, 6 + j])
            if j >= 2:
                ref = V.at[a, 4 * col(1) + j]
                pending.append(send(ref, ref, ags.at[a - 1, 8 + j], agr.at[a - 1, 8 + j], (t, col(-1))))
            add_product(a, [(col(-1), j), (col(1), j)], False)
        for f in (0, 1):
            arrived(V.at[a, 4 * col(2) + f], agr.at[a - 1, 4 + f])
            arrived(V.at[a, 4 * col(2) + 2 + f], agr.at[a - 1, 10 + f])
            add_product(a, [(col(2), f), (col(2), 2 + f)], False)

    def hidden_states(s):
        def tile(n, carry):
            cols = pl.ds(pl.multiple_of(n * 256, 256), 256)
            H[s, :, cols] = jax.nn.sigmoid(beta * acc[:, cols] + L[2 * s, :, cols]).astype(BF16)
            return carry

        lax.fori_loop(0, 4, tile, 0)

    def partial(s, b, j):
        return lax.dot_general(
            H[s], W[pl.ds(pl.multiple_of(b * BLK + j * CW, CW), CW), :], (((1,), (1,)), ((), ())),
            preferred_element_type=F32,
        )

    def order(i):
        return lax.rem(2 * i, 4) + lax.rem(i, 4) // 2

    def visible_states(s):
        def first(i, carry):
            g, j = i // 4, order(i)
            sg = 1 - 2 * (j // 2)
            b = jnp.where(g == 0, col(2), col(-sg))
            target = jnp.where(g == 0, col(sg), col(-sg))
            k = 4 * g + j
            SB[s, k] = partial(s, b, j).astype(BF16)
            send(SB.at[s, k], RB.at[s, k], rss.at[s, k], rsr.at[s, k], (t, target))
            return carry

        lax.fori_loop(0, 8, first, 0)

        def merge(i, carry):
            j = order(i)
            sg = 1 - 2 * (j // 2)
            term = partial(s, col(sg), j)
            arrived(RB.at[s, j], rsr.at[s, j])
            SB[s, 8 + j] = (term + RB[s, j].astype(F32)).astype(BF16)
            send(SB.at[s, 8 + j], RB.at[s, 8 + j], rss.at[s, 8 + j], rsr.at[s, 8 + j], (t, col(sg)))
            return carry

        lax.fori_loop(0, 4, merge, 0)

        def own(j, carry):
            PF[j] = partial(s, m, j)
            return carry

        lax.fori_loop(0, 4, own, 0)

        def last(i, carry):
            j = order(i)
            arrived(RB.at[s, 4 + j], rsr.at[s, 4 + j])
            arrived(RB.at[s, 8 + j], rsr.at[s, 8 + j])
            pre = PF[j] + RB[s, 4 + j].astype(F32) + RB[s, 8 + j].astype(F32)
            cols = pl.ds(pl.multiple_of(j * CW, CW), CW)
            V[s + 1, 4 * m + j] = jax.nn.sigmoid(beta * pre + L[2 * s + 1, :, cols]).astype(BF16)
            ref = V.at[s + 1, 4 * m + j]
            send(ref, ref, ags.at[s, j], agr.at[s, j], (t, col(1)))
            send(ref, ref, ags.at[s, 6 + j], agr.at[s, 6 + j], (t, col(-1)))
            return carry

        lax.fori_loop(0, 4, last, 0)

    add_product(0, [(b, j) for b in range(4) for j in range(4)], True)
    hidden_states(0)
    visible_states(0)
    gathered_product(1)
    hidden_states(1)
    for e in (0, 1):
        pending.append(send(H.at[1], swaph.at[e], sws.at[e], swr.at[e], (rep(1 - 2 * e), m)))
    visible_states(1)
    mine = V.at[2, pl.ds(4 * m, 4)]
    for e in (0, 1):
        pending.append(send(mine, swapv.at[e], sws.at[2 + e], swr.at[2 + e], (rep(1 - 2 * e), m)))

    gathered_product(2)

    def bias_part(g, total):
        return total + V[2, 4 * m + g // 2, :, pl.ds(pl.multiple_of(lax.rem(g, 2) * 128, 128), 128)].astype(F32) * vbias[
            m, :, pl.ds(pl.multiple_of(g * 128, 128), 128)
        ]

    total = BT[...] * lax.fori_loop(0, 8, bias_part, jnp.zeros((ROWS, 128), F32))

    def soft_part(g, total):
        cols = pl.ds(pl.multiple_of(g * 128, 128), 128)
        x = BT[...] * (acc[:, cols] + hbias[:, cols])
        return total + (jnp.maximum(x, 0.0) + jnp.log1p(jnp.exp(-jnp.abs(x))))

    total = lax.fori_loop(0, 8, soft_part, total)
    ebuf[0, m] = jnp.zeros((8, 128), F32)
    for h in (0, 1):
        ebuf[0, m, h : h + 1, :] = jnp.sum(total[128 * h : 128 * h + 128, :].T, axis=0, keepdims=True) * (-1.0 / NH)
    targets = [(0, d) for d in (1, 2, 3)] + [(e, d) for e in (1, -1) for d in range(4)]
    for e, d in targets:
        i = (e % 3) * 4 + d
        pending.append(send(ebuf.at[0, m], ebuf.at[e % 3, m], es.at[i], er.at[i], (rep(e), col(d))))

    for e in (0, 1):
        arrived(swaph.at[e], swr.at[e])

    def swap_hidden(g, carry):
        cols = pl.ds(pl.multiple_of(g * 128, 128), 128)
        low, up, own = swaph[0, :, cols].astype(F32), swaph[1, :, cols].astype(F32), H[1, :, cols].astype(F32)
        ho[:, cols] = jnp.where(TU[...] > 0.5, up, jnp.where(TL[...] > 0.5, low, own)).astype(BF16)
        return carry

    lax.fori_loop(0, 8, swap_hidden, 0)
    hput = pltpu.make_async_copy(ho, hid_out, lsem.at[9])
    hput.start()
    for e in (0, 1):
        arrived(swapv.at[e], swr.at[2 + e])

    def swap_visible(g, carry):
        cols = pl.ds(pl.multiple_of(lax.rem(g, 2) * 128, 128), 128)
        k = g // 2
        low, up = swapv[0, k, :, cols].astype(F32), swapv[1, k, :, cols].astype(F32)
        own = V[2, 4 * m + k, :, cols].astype(F32)
        vo[:, pl.ds(pl.multiple_of(g * 128, 128), 128)] = jnp.where(
            TU[...] > 0.5, up, jnp.where(TL[...] > 0.5, low, own)
        ).astype(BF16)
        return carry

    lax.fori_loop(0, 8, swap_visible, 0)
    vput = pltpu.make_async_copy(vo, vis_out, lsem.at[10])
    vput.start()
    for e, d in targets:
        arrived(ebuf.at[e % 3, col(-d)], er.at[(e % 3) * 4 + d])

    def summed(k):
        return ebuf[k, 0, 0:2, :] + ebuf[k, 1, 0:2, :] + ebuf[k, 2, 0:2, :] + ebuf[k, 3, 0:2, :]

    energy_out[...] = jnp.where(take_up > 0.5, summed(2), jnp.where(take_low > 0.5, summed(1), summed(0)))

    for copy in pending:
        copy.wait_send()
    arrived(half, dsem.at[0])
    for s in range(SWEEPS):

        def left(k, carry):
            arrived(SB.at[s, k], rss.at[s, k])
            return carry

        lax.fori_loop(0, 12, left, 0)
        for j in range(4):
            arrived(V.at[s + 1, j], ags.at[s, j])
            arrived(V.at[s + 1, j], ags.at[s, 6 + j])
    hput.wait()
    vput.wait()


def on_device(
    chains, weights, visible_bias, hidden_bias, inv_temps, hidden_thresholds, visible_thresholds, swap_phase, swap_accept
):
    vmem = pl.BlockSpec(memory_space=pltpu.VMEM)
    hbm = pl.BlockSpec(memory_space=pl.ANY)
    dma = pltpu.SemaphoreType.DMA
    n = len(MSGS)
    vis, hid, energy = pl.pallas_call(
        kernel,
        out_shape=(
            jax.ShapeDtypeStruct((ROWS, BLK), BF16),
            jax.ShapeDtypeStruct((ROWS, BLK), BF16),
            jax.ShapeDtypeStruct((2, 128), F32),
        ),
        in_specs=[hbm, hbm, vmem, vmem, vmem, hbm, hbm, vmem, vmem],
        out_specs=(hbm, hbm, vmem),
        scratch_shapes=[
            pltpu.VMEM((4096, BLK), BF16),
            pltpu.VMEM((3, 16, ROWS, CW), BF16),
            pltpu.VMEM((4, ROWS, BLK), jnp.int32),
            pltpu.VMEM((4, ROWS, BLK), F32),
            pltpu.VMEM((ROWS, BLK), F32),
            pltpu.VMEM((2, ROWS, BLK), BF16),
            pltpu.VMEM((2, 12, ROWS, CW), BF16),
            pltpu.VMEM((2, 12, ROWS, CW), BF16),
            pltpu.VMEM((4, ROWS, CW), F32),
            pltpu.VMEM((8, 128), F32),
            pltpu.VMEM((2, 8, 128), F32),
            pltpu.VMEM((2, 4, ROWS, CW), BF16),
            pltpu.VMEM((2, ROWS, BLK), BF16),
            pltpu.VMEM((ROWS, BLK), BF16),
            pltpu.VMEM((ROWS, BLK), BF16),
            pltpu.VMEM((ROWS, 128), F32),
            pltpu.VMEM((ROWS, 128), F32),
            pltpu.VMEM((ROWS, 128), F32),
            pltpu.VMEM((3, 4, 8, 128), F32),
            dma((n,)), dma((n,)), dma((2,)),
            dma((2, 12)), dma((2, 12)), dma((2, 12)), dma((2, 12)),
            dma((4,)), dma((4,)), dma((2,)), dma((2,)), dma((12,)), dma((12,)), dma((11,)),
        ],
        compiler_params=pltpu.CompilerParams(
            collective_id=0, has_side_effects=True, vmem_limit_bytes=58 * 2**20
        ),
        name="tempered",
    )(
        chains,
        weights,
        visible_bias.reshape(4, 1, BLK),
        hidden_bias.reshape(1, BLK),
        inv_temps.reshape(1, 1),
        hidden_thresholds,
        visible_thresholds,
        swap_phase.reshape(2, 128),
        swap_accept.reshape(2, 128),
    )
    return vis, hid, energy.reshape(ROWS)


def solution(mesh):
    return jax.shard_map(
        on_device,
        mesh=mesh,
        in_specs=(
            P("temp", "mp"),
            P("temp", "mp"),
            P(),
            P("mp"),
            P("temp"),
            P(None, "temp", "mp"),
            P(None, "temp", None),
            P(),
            P("temp"),
        ),
        out_specs=(P("temp", "mp"), P("temp", "mp"), P("temp")),
        check_vma=False,
    )
```

```python
import heapq

import jax
import jax.numpy as jnp
from jax import lax
from jax.experimental import pallas as pl
from jax.experimental.pallas import tpu as pltpu
from jax.sharding import PartitionSpec as P

NH = 4096
SWEEPS = 2
NY, NZ, NX, NT = 4, 8, 4, 64
ROWS, HALF, BLK, CW = 256, 128, 1024, 256
F32, BF16, I32 = jnp.float32, jnp.bfloat16, jnp.int32
MESH = pl.DeviceIdType.MESH
FIRST = (24, 24)


def gather_plan(p):
    na = FIRST[p]
    nb = 64 - na
    ha, hb = (na // 2 + 7) // 8 * 8, (nb // 2 + 7) // 8 * 8
    own = [] if p == 0 else [(1, "XW")]
    msgs = []

    def add(name, step, owner, first, rows, deps):
        msgs.append(((p, *name), step, owner, first, rows, [d if d in own else (p, *d) for d in deps] if deps else own))

    for d in range(1, 5):
        for s in (1, -1):
            first, rows = (na, nb) if d < 4 else ((na, hb) if s > 0 else (na + hb, nb - hb))
            add(("BZ", s, d), (0, s), (0, -s * (d - 1)), first, rows, [("BZ", s, d - 1)] if d > 1 else [])
    add(("AY", 1, 1), (1, 0), (0, 0), 0, na, [])
    add(("AY", -1, 1), (-1, 0), (0, 0), 0, na, [])
    add(("AY", 1, 2), (1, 0), (-1, 0), 0, ha, [("AY", 1, 1)])
    add(("AY", -1, 2), (-1, 0), (1, 0), ha, na - ha, [("AY", -1, 1)])
    there = ([], [("AY", 1, 1)], [("AY", -1, 1)], [("AY", 1, 2), ("AY", -1, 2)])
    for d in range(1, 5):
        for j, oy in enumerate((0, -1, 1, 2)):
            for s in (1, -1):
                if d == 4 and (j < 2) != (s > 0):
                    continue
                deps = there[j] if d == 1 else [("AZ", s, d - 1, j)]
                add(("AZ", s, d, j), (0, s), (oy, -s * (d - 1)), 0, na, deps)
    for zz in (0, -1, 1, -2, 2, -3, 3, 4):
        deps = [] if zz == 0 else ([("BZ", 1, 4), ("BZ", -1, 4)] if zz == 4 else [("BZ", -1 if zz > 0 else 1, abs(zz))])
        for s in (1, -1):
            add(("BY", s, 1, zz), (s, 0), (0, zz), na, nb, deps)
        s = 1 if zz in (0, 1, -2, 3) else -1
        add(("BY", s, 2, zz), (s, 0), (-s, zz), na, nb, [("BY", s, 1, zz)])
    return msgs


def arrival_order(msgs):
    free, done, left = {}, set(), list(msgs)
    events, sends, waits = [(9.0, -1, (1, "XW"))], {}, []

    def issue(now):
        out = []
        for m in list(left):
            ahead = 1.5 if m[0][0] and any(o[0][0] == 0 and o[1] == m[1] for o in left) else 3.0
            if all(d in done for d in m[5]) and free.get(m[1], 0.0) - now < ahead:
                left.remove(m)
                begin = max(now, free.get(m[1], 0.0))
                free[m[1]] = begin + 1.4 * m[4] / 32
                heapq.heappush(events, (free[m[1]] + 2.2, len(msgs) - len(left), m[0]))
                out.append(m[0])
        return out

    sends[None] = issue(0.0)
    while events:
        now, _, name = heapq.heappop(events)
        done.add(name)
        waits.append(name)
        sends[name] = issue(now)
    assert not left
    return sends, waits


MSGS = gather_plan(0) + gather_plan(1)
INDEX = {m[0]: i for i, m in enumerate(MSGS)}
SENDS, WAITS = arrival_order(MSGS)
LAST0 = max(n for n, name in enumerate(WAITS) if name[0] == 0)


def kernel(
    chains, weights, vbias, hbias, temps, hthr, vthr, phase, accept,
    vis_out, hid_out, energy_out,
    W, V, CO, thr, TS, TR, hbr, L, acc, PA, H, HX, VX, SB, RB, meta, metar, swapv, swaph, vo, ho, BT, TU, TL, ebuf,
    gs, gr, dsem, xs, xr, ags, agr, rss, rsr, fs, fr, sws, swr, ms, mr, es, er, lsem,
):
    t = lax.axis_index("temp")
    m = lax.axis_index("mp")
    c = lax.rem(t, 2)
    z = lax.rem(t // 2, NZ)
    y = t // (2 * NZ)

    def col(d):
        return lax.rem(m + d + NX, NX)

    def rep(d):
        return lax.rem(t + d + NT, NT)

    def temp_of(dy, dz):
        return (lax.rem(y + dy + NY, NY) * NZ + lax.rem(z + dz + NZ, NZ)) * 2 + c

    step = 1 - 2 * lax.rem(m + c, 2)
    partner, other, far = (t, col(step)), (t, col(-step)), (t, col(2))
    a = lax.rem(m - c + NX, NX) // 2
    mine = pl.ds(pl.multiple_of(a * HALF, HALF), HALF)
    theirs = pl.ds(pl.multiple_of((1 - a) * HALF, HALF), HALF)

    def units(s, half, mate=False):
        if half:
            return col(step) if mate else m
        if s < SWEEPS - 1:
            return col(step + 2) if mate else col(2)
        return col(2) if mate else col(-step)

    pending = []

    def send(src, dst, ssem, rsem, device):
        copy = pltpu.make_async_remote_copy(
            src_ref=src, dst_ref=dst, send_sem=ssem, recv_sem=rsem, device_id=device, device_id_type=MESH
        )
        copy.start()
        return copy

    def arrived(ref, sem):
        pltpu.make_async_copy(ref, ref, sem).wait()

    def load(src, dst, i):
        copy = pltpu.make_async_copy(src, dst, lsem.at[i])
        copy.start()
        return copy

    block = pl.ds(pl.multiple_of(t * 64, 64), 64)
    wload = load(weights, W.at[0, block], 0)
    vload = [load(chains.at[mine, pl.ds(j * CW, CW)], V.at[0, 4 * m + j], 1 + j) for j in range(4)]
    oload = [load(chains.at[theirs, pl.ds(j * CW, CW)], CO.at[j], 5 + j) for j in range(4)]
    tload = {}
    for s in range(SWEEPS):
        tload[2 * s, 1] = load(hthr.at[s, theirs], thr.at[2 * s, 1], 9 + 4 * s)
        tload[2 * s, 0] = load(hthr.at[s, mine], thr.at[2 * s, 0], 10 + 4 * s)
        for p in range(2):
            cols = pl.ds(pl.multiple_of(units(s, 1 - p) * BLK, BLK), BLK)
            tload[2 * s + 1, p] = load(vthr.at[s, mine, cols], thr.at[2 * s + 1, p], 11 + 4 * s + p)
    beta = temps[0:1, 0:1]
    meta[...] = jnp.broadcast_to(beta, (8, 128))
    meta[0:2, :] = accept[...].astype(F32)

    barrier = pltpu.get_barrier_semaphore()
    peers = [(t, col(1)), (t, col(-1)), (t, col(2)), (rep(1), m), (rep(-1), m)]
    peers += [(temp_of(1, 0), m), (temp_of(-1, 0), m), (temp_of(0, 1), m), (temp_of(0, -1), m)]
    for peer in peers:
        pl.semaphore_signal(barrier, inc=1, device_id=peer, device_id_type=MESH)
    pl.semaphore_wait(barrier, len(peers))

    sibling = (t + 1 - 2 * c, m)

    def place(name, seen):
        p = name[0]
        _, (sy, sz), (oy, oz), first, rows, _ = MSGS[INDEX[name]]
        start = temp_of(oy - (sy if seen else 0), oz - (sz if seen else 0)) * 64 + first
        return W.at[p, pl.ds(pl.multiple_of(start, 8), rows)]

    def launch(name):
        i = INDEX[name]
        ref = place(name, False)
        pending.append(send(ref, ref, gs.at[i], gr.at[i], (temp_of(*MSGS[i][1]), m)))

    def to_sibling(p, ref):
        send(ref, ref, dsem.at[p, 0], dsem.at[p, 1], sibling)

    wload.wait()
    for name in SENDS[None]:
        launch(name)
    pending.append(send(W.at[0, block], W.at[1, block], xs.at[0], xr.at[0], far))
    to_sibling(0, W.at[0, block])
    for cp in vload:
        cp.wait()
    own_v = V.at[0, pl.ds(4 * m, 4)]
    pending.append(send(own_v, own_v, xs.at[1], xr.at[1], partner))
    for cp in oload:
        cp.wait()
    pending.append(send(CO, own_v, xs.at[2], xr.at[2], other))
    pending.append(send(CO, own_v, xs.at[3], xr.at[3], far))
    pending.append(send(hbias, hbr, xs.at[4], xr.at[4], far))
    for e in (0, 1):
        pending.append(send(meta, metar.at[e], ms.at[e], mr.at[e], (rep(1 - 2 * e), m)))

    def send_thresholds(s):
        tload[2 * s, 1].wait()
        TS[s] = thr[2 * s, 1].astype(F32).astype(BF16)
        pending.append(send(TS.at[s], TR.at[s], xs.at[5 + s], xr.at[5 + s], far))

    def prepare(k, p):
        if k % 2 == 0 and p == 1:
            arrived(TR.at[k // 2], xr.at[5 + k // 2])
            if k == 0:
                arrived(hbr, xr.at[4])
        else:
            tload[k, p].wait()

        def some(i, carry):
            r = pl.ds(pl.multiple_of(i * 32, 32), 32)
            if k % 2 == 0 and p == 1:
                value, bias = TR[k // 2, r, :], hbr[...]
            else:
                value, bias = thr[k, p, r, :], (hbias[...] if k % 2 == 0 else vbias[units(k // 2, 1 - p)])
            level = (value.astype(F32) + 0.5) / 256.0
            L[k, p, r, :] = beta * bias + (jnp.log(level) - jnp.log(1.0 - level))
            return carry

        lax.fori_loop(0, HALF // 32, some, 0)

    def decisions():
        for e in (0, 1):
            arrived(metar.at[e], mr.at[e])
        low, up = metar.at[0], metar.at[1]
        ph = phase[...]
        lower = (lax.rem(t, 2) == ph) & (t + 1 < NT)
        upper = (lax.rem(t + 1, 2) == ph) & (t >= 1)
        take_up = jnp.where(lower & (accept[...] == 1), 1.0, 0.0)
        take_low = jnp.where(upper & (low[0:2, :] > 0.5), 1.0, 0.0)
        b = jnp.where(take_up > 0.5, up[2:4, :], jnp.where(take_low > 0.5, low[2:4, :], jnp.broadcast_to(beta, (2, 128))))
        for h in (0, 1):
            for ref, rows in ((TU, take_up), (TL, take_low)):
                ref[128 * h : 128 * h + 128, :] = jnp.broadcast_to(rows[h : h + 1, :], (128, 128)).T
        BT[...] = jnp.broadcast_to(jnp.where(a == 0, b[0:1, :], b[1:2, :]), (128, 128)).T
        return take_up, take_low

    def dot(x, w):
        return jnp.dot(x, w, preferred_element_type=F32)

    def dot_t(x, w):
        return lax.dot_general(x, w, (((1,), (1,)), ((), ())), preferred_element_type=F32)

    def wrows(k):
        return pl.ds(pl.multiple_of(k * CW, CW), CW)

    def add_product(ph, p, chunks, fresh):
        for n in range(4):
            cols = pl.ds(n * CW, CW)
            total = None
            for k in chunks:
                part = dot(V[ph, k], W[p, wrows(k), cols])
                total = part if total is None else total + part
            acc[p, :, cols] = total if fresh else acc[p, :, cols] + total

    def hidden_states(s, p):
        def tile(n, carry):
            cols = pl.ds(pl.multiple_of(n * CW, CW), CW)
            H[s, p, :, cols] = jax.nn.sigmoid(beta * acc[p, :, cols] + L[2 * s, p, :, cols]).astype(BF16)
            return carry

        lax.fori_loop(0, 4, tile, 0)

    def first_half():
        half0 = W.at[0, pl.ds(0, NT // 2 * 64)]
        arrived(half0, dsem.at[0, 1])
        arrived(own_v, xr.at[1])
        arrived(own_v, xr.at[2])
        arrived(own_v, xr.at[3])
        add_product(0, 0, range(16), True)
        hidden_states(0, 0)

    def first_partials(g):
        def tile(j, carry):
            PA[4 * g + j] = dot_t(H[0, 0], W[0, wrows(4 * g + j), :])
            return carry

        lax.fori_loop(0, 4, tile, 0)

    flags = None
    early = [lambda: send_thresholds(0), lambda: send_thresholds(1)]
    early += [lambda k=k, p=p: prepare(k, p) for k, p in ((0, 0), (1, 0), (1, 1), (2, 0), (3, 0), (3, 1))]
    late = [first_half] + [lambda g=g: first_partials(g) for g in range(4)]
    late += [lambda: prepare(0, 1), lambda: prepare(2, 1)]
    for n, name in enumerate(WAITS):
        if name[1] == "XW":
            ref = W.at[1, block]
            arrived(ref, xr.at[0])
        else:
            ref = place(name, True)
            arrived(ref, gr.at[INDEX[name]])
        for nxt in SENDS[name]:
            launch(nxt)
        to_sibling(name[0], ref)
        if n >= 4 and n % 3 == 0 and early:
            early.pop(0)()
        if n == 32:
            flags = decisions()
        if n >= LAST0 + 2 and (n - LAST0) % 3 == 0 and late:
            late.pop(0)()
    for job in early + late:
        job()
    take_up, take_low = flags
    arrived(W.at[1, pl.ds(0, NT // 2 * 64)], dsem.at[1, 1])

    def partial(s, k):
        if s == 0:
            return PA[k] + dot_t(H[0, 1], W[1, wrows(k), :])
        return dot_t(H[s, 0], W[0, wrows(k), :]) + dot_t(H[s, 1], W[1, wrows(k), :])

    def visible_states(s):
        def give(h, carry):
            terms = []
            for i in (2 * h, 2 * h + 1):
                q = jnp.where(h < 2, units(s, 0, True), units(s, 1, True))
                terms.append(partial(s, 4 * q + lax.rem(i, 4)))
            for e in (0, 1):
                i = 2 * h + e
                SB[s, i] = terms[e].astype(BF16)
                send(SB.at[s, i], RB.at[s, i], rss.at[s, i], rsr.at[s, i], partner)
            return carry

        lax.fori_loop(0, 4, give, 0)

        def keep(half):
            def two(h, carry):
                own = [partial(s, 4 * units(s, half) + 2 * h + e) for e in (0, 1)]
                for e in (0, 1):
                    j = 2 * h + e
                    i = 4 * half + j
                    k = 4 * units(s, half) + j
                    arrived(RB.at[s, i], rsr.at[s, i])
                    cols = pl.ds(pl.multiple_of(j * CW, CW), CW)
                    pre = own[e] + RB[s, i].astype(F32)
                    V[s + 1, k] = jax.nn.sigmoid(beta * pre + L[2 * s + 1, 1 - half, :, cols]).astype(BF16)
                    ref = V.at[s + 1, k]
                    send(ref, ref, ags.at[s, i], agr.at[s, i], partner)
                    if s == SWEEPS - 1 and half == 0:
                        send(ref, VX.at[j], fs.at[1 + j], fr.at[1 + j], other)
                return carry

            lax.fori_loop(0, 2, two, 0)

        keep(0)
        keep(1)

    def gathered_product(ph):
        own = [4 * units(ph - 1, i // 4) + i % 4 for i in range(8)]
        for p in (0, 1):
            add_product(ph, p, own, True)
        for i in range(0, 8, 2):
            ks = [4 * units(ph - 1, i // 4, True) + i % 4 + e for e in (0, 1)]
            for e in (0, 1):
                arrived(V.at[ph, ks[e]], agr.at[ph - 1, i + e])
            for p in (0, 1):
                add_product(ph, p, ks, False)
            if ph == SWEEPS:
                swap_far(i // 2)

    def swap_far(j):
        arrived(VX.at[j], fr.at[1 + j])
        for e in (0, 1):
            ref = swapv.at[e, 1 - a, j]
            pending.append(send(VX.at[j], ref, sws.at[3 + j, e], swr.at[3 + j, e], (rep(1 - 2 * e), m)))

    add_product(0, 1, range(16), True)
    hidden_states(0, 1)
    visible_states(0)
    gathered_product(1)
    for p in (1, 0):
        hidden_states(1, p)
    pending.append(send(H.at[1, 1], HX, fs.at[0], fr.at[0], far))
    for e in (0, 1):
        pending.append(send(H.at[1, 0], swaph.at[e, a], sws.at[0, e], swr.at[0, e], (rep(1 - 2 * e), m)))
    visible_states(1)
    own_out = V.at[2, pl.ds(4 * m, 4)]
    for e in (0, 1):
        pending.append(send(own_out, swapv.at[e, a], sws.at[1, e], swr.at[1, e], (rep(1 - 2 * e), m)))
    arrived(HX, fr.at[0])
    for e in (0, 1):
        pending.append(send(HX, swaph.at[e, 1 - a], sws.at[2, e], swr.at[2, e], (rep(1 - 2 * e), m)))

    gathered_product(2)
    def lanes(g):
        return pl.ds(pl.multiple_of(g * 128, 128), 128)

    total = jnp.zeros((HALF, 128), F32)
    for p in (0, 1):
        q = units(SWEEPS - 1, 1 - p)

        def bias_part(g, value):
            return value + V[2, 4 * q + g // 2, :, lanes(lax.rem(g, 2))].astype(F32) * vbias[q, :, lanes(g)]

        total = lax.fori_loop(0, 8, bias_part, total)
    total = BT[...] * total
    for p in (0, 1):
        bias_ref = hbr if p else hbias

        def soft_part(g, value):
            x = BT[...] * (acc[p, :, lanes(g)] + bias_ref[:, lanes(g)])
            return value + (jnp.maximum(x, 0.0) + jnp.log1p(jnp.exp(-jnp.abs(x))))

        total = lax.fori_loop(0, 8, soft_part, total)
    ebuf[0, m] = jnp.broadcast_to(jnp.sum(total.T, axis=0, keepdims=True) * (-1.0 / NH), (8, 128))
    targets = [(0, d) for d in (1, 2, 3)] + [(e, d) for e in (1, -1) for d in range(4)]
    for e, d in targets:
        i = (e % 3) * 4 + d
        pending.append(send(ebuf.at[0, m], ebuf.at[e % 3, m], es.at[i], er.at[i], (rep(e), col(d))))

    for e in (0, 1):
        arrived(swaph.at[e, 0], swr.at[0, e])
        arrived(swaph.at[e, 1], swr.at[2, e])

    def chosen(rows, up, low, own):
        value = jnp.where(TL[rows, :] > 0.5, low.astype(F32), own.astype(F32))
        return jnp.where(TU[rows, :] > 0.5, up.astype(F32), value).astype(BF16)

    def swap_hidden(g, carry):
        cols = lanes(g)
        ho[mine, cols] = chosen(mine, swaph[1, a, :, cols], swaph[0, a, :, cols], H[1, 0, :, cols])
        ho[theirs, cols] = chosen(theirs, swaph[1, 1 - a, :, cols], swaph[0, 1 - a, :, cols], HX[:, cols])
        return carry

    lax.fori_loop(0, 8, swap_hidden, 0)
    hput = load(ho, hid_out, 17)
    for e in (0, 1):
        arrived(swapv.at[e, 0], swr.at[1, e])
        for j in range(4):
            arrived(swapv.at[e, 0, j], swr.at[3 + j, e])

    def swap_visible(g, carry):
        k, cols, out = g // 2, lanes(lax.rem(g, 2)), lanes(g)
        vo[mine, out] = chosen(mine, swapv[1, a, k, :, cols], swapv[0, a, k, :, cols], V[2, 4 * m + k, :, cols])
        vo[theirs, out] = chosen(theirs, swapv[1, 1 - a, k, :, cols], swapv[0, 1 - a, k, :, cols], VX[k, :, cols])
        return carry

    lax.fori_loop(0, 8, swap_visible, 0)
    vput = load(vo, vis_out, 18)
    for e, d in targets:
        arrived(ebuf.at[e % 3, col(-d)], er.at[(e % 3) * 4 + d])

    def summed(k):
        parity = c if k == 0 else 1 - c
        low = ebuf[k, parity, 0:1, :] + ebuf[k, parity + 1, 0:1, :]
        high = ebuf[k, parity + 2, 0:1, :] + ebuf[k, lax.rem(parity + 3, NX), 0:1, :]
        return low, high

    sums = [summed(k) for k in range(3)]
    for h in (0, 1):
        value = jnp.where(take_low[h : h + 1] > 0.5, sums[1][h], sums[0][h])
        energy_out[h : h + 1, :] = jnp.where(take_up[h : h + 1] > 0.5, sums[2][h], value)

    for copy in pending:
        copy.wait_send()
    for p in (0, 1):
        arrived(W.at[p, pl.ds(0, NT // 2 * 64)], dsem.at[p, 0])
    for s in range(SWEEPS):

        def left(i, carry):
            arrived(SB.at[s, i], rss.at[s, i])
            arrived(V.at[s + 1, i], ags.at[s, i])
            return carry

        lax.fori_loop(0, 8, left, 0)
    for j in range(4):
        arrived(VX.at[j], fs.at[1 + j])
    hput.wait()
    vput.wait()


def on_device(
    chains, weights, visible_bias, hidden_bias, inv_temps, hidden_thresholds, visible_thresholds, swap_phase, swap_accept
):
    vmem = pl.BlockSpec(memory_space=pltpu.VMEM)
    hbm = pl.BlockSpec(memory_space=pl.ANY)
    dma, mem = pltpu.SemaphoreType.DMA, pltpu.VMEM
    n = len(MSGS)
    vis, hid, energy = pl.pallas_call(
        kernel,
        out_shape=(
            jax.ShapeDtypeStruct((ROWS, BLK), BF16),
            jax.ShapeDtypeStruct((ROWS, BLK), BF16),
            jax.ShapeDtypeStruct((2, 128), F32),
        ),
        in_specs=[hbm, hbm, vmem, vmem, vmem, hbm, hbm, vmem, vmem],
        out_specs=(hbm, hbm, vmem),
        scratch_shapes=[
            mem((2, 4096, BLK), BF16),
            mem((3, 16, HALF, CW), BF16),
            mem((4, HALF, CW), BF16),
            mem((4, 2, HALF, BLK), I32),
            mem((2, HALF, BLK), BF16),
            mem((2, HALF, BLK), BF16),
            mem((1, BLK), F32),
            mem((4, 2, HALF, BLK), F32),
            mem((2, HALF, BLK), F32),
            mem((16, HALF, CW), F32),
            mem((2, 2, HALF, BLK), BF16),
            mem((HALF, BLK), BF16),
            mem((4, HALF, CW), BF16),
            mem((2, 8, HALF, CW), BF16),
            mem((2, 8, HALF, CW), BF16),
            mem((8, 128), F32),
            mem((2, 8, 128), F32),
            mem((2, 2, 4, HALF, CW), BF16),
            mem((2, 2, HALF, BLK), BF16),
            mem((ROWS, BLK), BF16),
            mem((ROWS, BLK), BF16),
            mem((HALF, 128), F32),
            mem((ROWS, 128), F32),
            mem((ROWS, 128), F32),
            mem((3, 4, 8, 128), F32),
            dma((n,)), dma((n,)), dma((2, 2)), dma((7,)), dma((7,)),
            dma((2, 8)), dma((2, 8)), dma((2, 8)), dma((2, 8)), dma((5,)), dma((5,)),
            dma((7, 2)), dma((7, 2)), dma((2,)), dma((2,)), dma((12,)), dma((12,)), dma((19,)),
        ],
        compiler_params=pltpu.CompilerParams(
            collective_id=0, has_side_effects=True, vmem_limit_bytes=58 * 2**20
        ),
        name="tempered",
    )(
        chains,
        weights,
        visible_bias.reshape(4, 1, BLK),
        hidden_bias.reshape(1, BLK),
        inv_temps.reshape(1, 1),
        hidden_thresholds,
        visible_thresholds,
        swap_phase.reshape(2, 128),
        swap_accept.reshape(2, 128),
    )
    return vis, hid, energy.reshape(ROWS)


def solution(mesh):
    return jax.shard_map(
        on_device,
        mesh=mesh,
        in_specs=(
            P("temp", "mp"),
            P("temp", "mp"),
            P(),
            P("mp"),
            P("temp"),
            P(None, "temp", "mp"),
            P(None, "temp", None),
            P(),
            P("temp"),
        ),
        out_specs=(P("temp", "mp"), P("temp", "mp"), P("temp")),
        check_vma=False,
    )
```

```python
import heapq

import jax
import jax.numpy as jnp
from jax import lax
from jax.experimental import pallas as pl
from jax.experimental.pallas import tpu as pltpu
from jax.sharding import PartitionSpec as P

NH = 4096
SWEEPS = 2
NY, NZ, NX, NT = 4, 8, 4, 64
ROWS, HALF, BLK, CW = 256, 128, 1024, 256
F32, BF16, I32 = jnp.float32, jnp.bfloat16, jnp.int32
MESH = pl.DeviceIdType.MESH
FIRST = (24, 24)


def gather_plan(p):
    na = FIRST[p]
    nb = 64 - na
    ha, hb = (na // 2 + 7) // 8 * 8, (nb // 2 + 7) // 8 * 8
    own = [] if p == 0 else [(1, "XW")]
    msgs = []

    def add(name, step, owner, first, rows, deps):
        msgs.append(((p, *name), step, owner, first, rows, [d if d in own else (p, *d) for d in deps] if deps else own))

    for d in range(1, 5):
        for s in (1, -1):
            first, rows = (na, nb) if d < 4 else ((na, hb) if s > 0 else (na + hb, nb - hb))
            add(("BZ", s, d), (0, s), (0, -s * (d - 1)), first, rows, [("BZ", s, d - 1)] if d > 1 else [])
    add(("AY", 1, 1), (1, 0), (0, 0), 0, na, [])
    add(("AY", -1, 1), (-1, 0), (0, 0), 0, na, [])
    add(("AY", 1, 2), (1, 0), (-1, 0), 0, ha, [("AY", 1, 1)])
    add(("AY", -1, 2), (-1, 0), (1, 0), ha, na - ha, [("AY", -1, 1)])
    there = ([], [("AY", 1, 1)], [("AY", -1, 1)], [("AY", 1, 2), ("AY", -1, 2)])
    for d in range(1, 5):
        for j, oy in enumerate((0, -1, 1, 2)):
            for s in (1, -1):
                if d == 4 and (j < 2) != (s > 0):
                    continue
                deps = there[j] if d == 1 else [("AZ", s, d - 1, j)]
                add(("AZ", s, d, j), (0, s), (oy, -s * (d - 1)), 0, na, deps)
    for zz in (0, -1, 1, -2, 2, -3, 3, 4):
        deps = [] if zz == 0 else ([("BZ", 1, 4), ("BZ", -1, 4)] if zz == 4 else [("BZ", -1 if zz > 0 else 1, abs(zz))])
        for s in (1, -1):
            add(("BY", s, 1, zz), (s, 0), (0, zz), na, nb, deps)
        s = 1 if zz in (0, 1, -2, 3) else -1
        add(("BY", s, 2, zz), (s, 0), (-s, zz), na, nb, [("BY", s, 1, zz)])
    return msgs


def arrival_order(msgs):
    free, done, left = {}, set(), list(msgs)
    events, sends, waits = [(9.0, -1, (1, "XW"))], {}, []

    def issue(now):
        out = []
        for m in list(left):
            ahead = 1.5 if m[0][0] and any(o[0][0] == 0 and o[1] == m[1] for o in left) else 3.0
            if all(d in done for d in m[5]) and free.get(m[1], 0.0) - now < ahead:
                left.remove(m)
                begin = max(now, free.get(m[1], 0.0))
                free[m[1]] = begin + 1.4 * m[4] / 32
                heapq.heappush(events, (free[m[1]] + 2.2, len(msgs) - len(left), m[0]))
                out.append(m[0])
        return out

    sends[None] = issue(0.0)
    while events:
        now, _, name = heapq.heappop(events)
        done.add(name)
        waits.append(name)
        sends[name] = issue(now)
    assert not left
    return sends, waits


MSGS = gather_plan(0) + gather_plan(1)
INDEX = {m[0]: i for i, m in enumerate(MSGS)}
SENDS, WAITS = arrival_order(MSGS)
LAST0 = max(n for n, name in enumerate(WAITS) if name[0] == 0)


def kernel(
    chains, weights, vbias, hbias, temps, hthr, vthr, phase, accept,
    vis_out, hid_out, energy_out,
    W, V, CO, thr, TS, TR, hbr, L, acc, PA, H, HX, VX, SB, RB, meta, metar, swapv, swaph, BT, TU, TL, ebuf,
    gs, gr, dsem, xs, xr, ags, agr, rss, rsr, fs, fr, sws, swr, ms, es, lsem,
):
    t = lax.axis_index("temp")
    m = lax.axis_index("mp")
    c = lax.rem(t, 2)
    z = lax.rem(t // 2, NZ)
    y = t // (2 * NZ)

    def col(d):
        return lax.rem(m + d + NX, NX)

    def rep(d):
        return lax.rem(t + d + NT, NT)

    def temp_of(dy, dz):
        return (lax.rem(y + dy + NY, NY) * NZ + lax.rem(z + dz + NZ, NZ)) * 2 + c

    step = 1 - 2 * lax.rem(m + c, 2)
    partner, other, far = (t, col(step)), (t, col(-step)), (t, col(2))
    a = lax.rem(m - c + NX, NX) // 2
    mine = pl.ds(pl.multiple_of(a * HALF, HALF), HALF)
    theirs = pl.ds(pl.multiple_of((1 - a) * HALF, HALF), HALF)

    def units(s, half, mate=False):
        if half:
            return col(step) if mate else m
        if s < SWEEPS - 1:
            return col(step + 2) if mate else col(2)
        return col(2) if mate else col(-step)

    def send(src, dst, ssem, rsem, device):
        copy = pltpu.make_async_remote_copy(
            src_ref=src, dst_ref=dst, send_sem=ssem, recv_sem=rsem, device_id=device, device_id_type=MESH
        )
        copy.start()

    def arrived(ref, sem):
        pltpu.make_async_copy(ref, ref, sem).wait()

    def load(src, dst, i):
        copy = pltpu.make_async_copy(src, dst, lsem.at[i])
        copy.start()
        return copy

    block = pl.ds(pl.multiple_of(t * 64, 64), 64)
    wload = load(weights, W.at[0, block], 0)
    vload = [load(chains.at[mine, pl.ds(j * CW, CW)], V.at[0, 4 * m + j], 1 + j) for j in range(4)]
    oload = [load(chains.at[theirs, pl.ds(j * CW, CW)], CO.at[j], 5 + j) for j in range(4)]
    tload = {}
    for s in range(SWEEPS):
        tload[2 * s, 1] = load(hthr.at[s, theirs], thr.at[2 * s, 1], 9 + 4 * s)
        tload[2 * s, 0] = load(hthr.at[s, mine], thr.at[2 * s, 0], 10 + 4 * s)
        for p in range(2):
            cols = pl.ds(pl.multiple_of(units(s, 1 - p) * BLK, BLK), BLK)
            tload[2 * s + 1, p] = load(vthr.at[s, mine, cols], thr.at[2 * s + 1, p], 11 + 4 * s + p)
    beta = temps[0:1, 0:1]
    meta[...] = jnp.broadcast_to(beta, (8, 128))
    meta[0:2, :] = accept[...].astype(F32)

    barrier = pltpu.get_barrier_semaphore()
    peers = [(t, col(1)), (t, col(-1)), (t, col(2)), (rep(1), m), (rep(-1), m)]
    peers += [(temp_of(1, 0), m), (temp_of(-1, 0), m), (temp_of(0, 1), m), (temp_of(0, -1), m)]
    for peer in peers:
        pl.semaphore_signal(barrier, inc=1, device_id=peer, device_id_type=MESH)
    pl.semaphore_wait(barrier, len(peers))

    sibling = (t + 1 - 2 * c, m)

    def place(name, seen):
        p = name[0]
        _, (sy, sz), (oy, oz), first, rows, _ = MSGS[INDEX[name]]
        start = temp_of(oy - (sy if seen else 0), oz - (sz if seen else 0)) * 64 + first
        return W.at[p, pl.ds(pl.multiple_of(start, 8), rows)]

    def launch(name):
        i = INDEX[name]
        ref = place(name, False)
        send(ref, ref, gs.at[name[0]], gr.at[i], (temp_of(*MSGS[i][1]), m))

    def to_sibling(p, ref):
        send(ref, ref, dsem.at[p, 0], dsem.at[p, 1], sibling)

    wload.wait()
    for name in SENDS[None]:
        launch(name)
    send(W.at[0, block], W.at[1, block], xs.at[0], xr.at[0], far)
    to_sibling(0, W.at[0, block])
    for cp in vload:
        cp.wait()
    own_v = V.at[0, pl.ds(4 * m, 4)]
    send(own_v, own_v, xs.at[1], xr.at[1], partner)
    for cp in oload:
        cp.wait()
    send(CO, own_v, xs.at[1], xr.at[1], other)
    send(CO, own_v, xs.at[1], xr.at[1], far)
    send(hbias, hbr, xs.at[2], xr.at[2], far)
    for e in (0, 1):
        send(meta, metar.at[e], ms.at[0], ms.at[1], (rep(1 - 2 * e), m))

    def send_thresholds(s):
        tload[2 * s, 1].wait()
        TS[s] = thr[2 * s, 1].astype(F32).astype(BF16)
        send(TS.at[s], TR.at[s], xs.at[3], xr.at[3 + s], far)

    def prepare(k, p):
        if k % 2 == 0 and p == 1:
            arrived(TR.at[k // 2], xr.at[3 + k // 2])
            if k == 0:
                arrived(hbr, xr.at[2])
        else:
            tload[k, p].wait()

        def some(i, carry):
            r = pl.ds(pl.multiple_of(i * 32, 32), 32)
            if k % 2 == 0 and p == 1:
                value, bias = TR[k // 2, r, :], hbr[...]
            else:
                value, bias = thr[k, p, r, :], (hbias[...] if k % 2 == 0 else vbias[units(k // 2, 1 - p)])
            level = (value.astype(F32) + 0.5) / 256.0
            L[k, p, r, :] = beta * bias + (jnp.log(level) - jnp.log(1.0 - level))
            return carry

        lax.fori_loop(0, HALF // 32, some, 0)

    def decisions():
        arrived(metar, ms.at[1])
        low, up = metar.at[0], metar.at[1]
        ph = phase[...]
        lower = (lax.rem(t, 2) == ph) & (t + 1 < NT)
        upper = (lax.rem(t + 1, 2) == ph) & (t >= 1)
        take_up = jnp.where(lower & (accept[...] == 1), 1.0, 0.0)
        take_low = jnp.where(upper & (low[0:2, :] > 0.5), 1.0, 0.0)
        b = jnp.where(take_up > 0.5, up[2:4, :], jnp.where(take_low > 0.5, low[2:4, :], jnp.broadcast_to(beta, (2, 128))))
        for h in (0, 1):
            for ref, rows in ((TU, take_up), (TL, take_low)):
                ref[128 * h : 128 * h + 128, :] = jnp.broadcast_to(rows[h : h + 1, :], (128, 128)).T
        BT[...] = jnp.broadcast_to(jnp.where(a == 0, b[0:1, :], b[1:2, :]), (128, 128)).T
        return take_up, take_low

    def dot(x, w):
        return jnp.dot(x, w, preferred_element_type=F32)

    def dot_t(x, w):
        return lax.dot_general(x, w, (((1,), (1,)), ((), ())), preferred_element_type=F32)

    def wrows(k):
        return pl.ds(pl.multiple_of(k * CW, CW), CW)

    def add_product(ph, p, chunks, fresh):
        for n in range(4):
            cols = pl.ds(n * CW, CW)
            total = None
            for k in chunks:
                part = dot(V[ph, k], W[p, wrows(k), cols])
                total = part if total is None else total + part
            acc[p, :, cols] = total if fresh else acc[p, :, cols] + total

    def hidden_states(s, p):
        def tile(n, carry):
            cols = pl.ds(pl.multiple_of(n * CW, CW), CW)
            H[s, p, :, cols] = jax.nn.sigmoid(beta * acc[p, :, cols] + L[2 * s, p, :, cols]).astype(BF16)
            return carry

        lax.fori_loop(0, 4, tile, 0)

    def first_half():
        half0 = W.at[0, pl.ds(0, NT // 2 * 64)]
        arrived(half0, dsem.at[0, 1])
        arrived(V.at[0, pl.ds(0, 12)], xr.at[1])
        add_product(0, 0, range(16), True)
        hidden_states(0, 0)

    def first_partials(g):
        def tile(j, carry):
            PA[4 * g + j] = dot_t(H[0, 0], W[0, wrows(4 * g + j), :])
            return carry

        lax.fori_loop(0, 4, tile, 0)

    flags = None
    early = [lambda: send_thresholds(0), lambda: send_thresholds(1)]
    early += [lambda k=k, p=p: prepare(k, p) for k, p in ((0, 0), (1, 0), (1, 1), (2, 0), (3, 0), (3, 1))]
    late = [first_half] + [lambda g=g: first_partials(g) for g in range(4)]
    late += [lambda: prepare(0, 1), lambda: prepare(2, 1)]
    for n, name in enumerate(WAITS):
        if name[1] == "XW":
            ref = W.at[1, block]
            arrived(ref, xr.at[0])
        else:
            ref = place(name, True)
            arrived(ref, gr.at[INDEX[name]])
        for nxt in SENDS[name]:
            launch(nxt)
        to_sibling(name[0], ref)
        if n >= 4 and n % 3 == 0 and early:
            early.pop(0)()
        if n == 32:
            flags = decisions()
        if n >= LAST0 + 2 and (n - LAST0) % 3 == 0 and late:
            late.pop(0)()
    for job in early + late:
        job()
    take_up, take_low = flags
    arrived(W.at[1, pl.ds(0, NT // 2 * 64)], dsem.at[1, 1])

    def partial(s, k):
        if s == 0:
            return PA[k] + dot_t(H[0, 1], W[1, wrows(k), :])
        return dot_t(H[s, 0], W[0, wrows(k), :]) + dot_t(H[s, 1], W[1, wrows(k), :])

    def visible_states(s):
        def give(i, term):
            SB[s, i] = term.astype(BF16)
            send(SB.at[s, i], RB.at[s, i], rss.at[s], rsr.at[s, i], partner)

        def keep(i, own):
            j, half = i % 4, i // 4
            k = 4 * units(s, half) + j
            arrived(RB.at[s, i], rsr.at[s, i])
            pre = own + RB[s, i].astype(F32)
            V[s + 1, k] = jax.nn.sigmoid(beta * pre + L[2 * s + 1, 1 - half, :, j * CW : j * CW + CW]).astype(BF16)
            ref = V.at[s + 1, k]
            send(ref, ref, ags.at[s], agr.at[s, i], partner)
            if s < SWEEPS - 1:
                return
            if half == 0:
                send(ref, VX.at[j], fs.at[1], fr.at[1 + j], other)
                return
            swap(ref, lambda e: swapv.at[e, a, j], 1)

        jobs = [(give, i, 4 * units(s, i // 4, True) + i % 4) for i in range(8)]
        jobs += [(keep, i, 4 * units(s, i // 4) + i % 4) for i in range(8)]
        def terms(n):
            return [partial(s, jobs[n + e][2]) for e in (0, 1)]

        ahead = terms(0)
        for n in range(0, len(jobs), 2):
            now, ahead = ahead, (terms(n + 2) if n + 2 < len(jobs) else None)
            for e in (0, 1):
                job, i, _ = jobs[n + e]
                job(i, now[e])

    def swap(src, dst, kind):
        for e in (0, 1):

            @pl.when(t + 1 < NT if e == 0 else t >= 1)
            def _():
                send(src, dst(e), sws.at[kind, e], swr.at[kind, e], (rep(1 - 2 * e), m))

    def gathered_product(ph):
        own = [4 * units(ph - 1, i // 4) + i % 4 for i in range(8)]
        if ph == SWEEPS:
            swap_far(0)
        add_product(ph, 0, own, True)
        if ph == SWEEPS:
            swap_far(1)
        add_product(ph, 1, own, True)
        for i in range(0, 8, 2):
            ks = [4 * units(ph - 1, i // 4, True) + i % 4 + e for e in (0, 1)]
            for e in (0, 1):
                arrived(V.at[ph, ks[e]], agr.at[ph - 1, i + e])
            for p in (0, 1):
                add_product(ph, p, ks, False)
            if ph == SWEEPS and i < 4:
                swap_far(2 + i // 2)

    def swap_far(j):
        arrived(VX.at[j], fr.at[1 + j])
        swap(VX.at[j], lambda e: swapv.at[e, 1 - a, j], 1)

    add_product(0, 1, range(16), True)
    hidden_states(0, 1)
    visible_states(0)
    gathered_product(1)
    for p in (1, 0):
        hidden_states(1, p)
    send(H.at[1, 1], HX, fs.at[0], fr.at[0], far)
    swap(H.at[1, 0], lambda e: swaph.at[e, a], 0)
    visible_states(1)
    arrived(HX, fr.at[0])
    swap(HX, lambda e: swaph.at[e, 1 - a], 0)

    gathered_product(2)
    def lanes(g):
        return pl.ds(pl.multiple_of(g * 128, 128), 128)

    total = jnp.zeros((HALF, 128), F32)
    for p in (0, 1):
        q = units(SWEEPS - 1, 1 - p)

        def bias_part(g, value):
            return value + V[2, 4 * q + g // 2, :, lanes(lax.rem(g, 2))].astype(F32) * vbias[q, :, lanes(g)]

        total = lax.fori_loop(0, 8, bias_part, total)
    total = BT[...] * total
    for p in (0, 1):
        bias_ref = hbr if p else hbias

        def soft_part(g, value):
            x = BT[...] * (acc[p, :, lanes(g)] + bias_ref[:, lanes(g)])
            return value + (jnp.maximum(x, 0.0) + jnp.log1p(jnp.exp(-jnp.abs(x))))

        total = lax.fori_loop(0, 8, soft_part, total)
    ebuf[m] = jnp.broadcast_to(jnp.sum(total.T, axis=0, keepdims=True) * (-1.0 / NH), (8, 128))
    targets = [(0, d) for d in (1, 2, 3)] + [(e, d) for e in (1, -1) for d in range(4)]
    for e, d in targets:
        send(ebuf.at[m], ebuf.at[(e % 3) * NX + m], es.at[0], es.at[1], (rep(e), col(d)))

    def swapped(ref, kind):
        for e in (0, 1):
            there = t >= 1 if e == 0 else t + 1 < NT

            @pl.when(there)
            def _():
                arrived(ref.at[e], swr.at[kind, e])

            @pl.when(jnp.logical_not(there))
            def _():
                ref[e] = jnp.zeros(ref.shape[1:], BF16)

    swapped(swaph, 0)

    def chosen(rows, up, low, own):
        value = jnp.where(TL[rows, :] > 0.5, low.astype(F32), own.astype(F32))
        return jnp.where(TU[rows, :] > 0.5, up.astype(F32), value).astype(BF16)

    def swap_hidden(g, carry):
        cols = lanes(g)
        hid_out[mine, cols] = chosen(mine, swaph[1, a, :, cols], swaph[0, a, :, cols], H[1, 0, :, cols])
        hid_out[theirs, cols] = chosen(theirs, swaph[1, 1 - a, :, cols], swaph[0, 1 - a, :, cols], HX[:, cols])
        return carry

    lax.fori_loop(0, 8, swap_hidden, 0)
    swapped(swapv, 1)

    def swap_visible(g, carry):
        k, cols, out = g // 2, lanes(lax.rem(g, 2)), lanes(g)
        vis_out[mine, out] = chosen(mine, swapv[1, a, k, :, cols], swapv[0, a, k, :, cols], V[2, 4 * m + k, :, cols])
        vis_out[theirs, out] = chosen(theirs, swapv[1, 1 - a, k, :, cols], swapv[0, 1 - a, k, :, cols], VX[k, :, cols])
        return carry

    lax.fori_loop(0, 8, swap_visible, 0)
    arrived(ebuf.at[pl.ds(0, 11)], es.at[1])

    def summed(k):
        parity = c if k == 0 else 1 - c
        low = ebuf[k * NX + parity, 0:1, :] + ebuf[k * NX + parity + 1, 0:1, :]
        high = ebuf[k * NX + parity + 2, 0:1, :] + ebuf[k * NX + lax.rem(parity + 3, NX), 0:1, :]
        return low, high

    sums = [summed(k) for k in range(3)]
    for h in (0, 1):
        value = jnp.where(take_low[h : h + 1] > 0.5, sums[1][h], sums[0][h])
        energy_out[h : h + 1, :] = jnp.where(take_up[h : h + 1] > 0.5, sums[2][h], value)

    for p in (0, 1):
        arrived(W.at[p, pl.ds(0, 31 * 64)], gs.at[p])
        arrived(W.at[p, pl.ds(0, NT // 2 * 64)], dsem.at[p, 0])
    arrived(W.at[0, block], xs.at[0])
    arrived(V.at[0, pl.ds(0, 12)], xs.at[1])
    arrived(hbr, xs.at[2])
    arrived(TR, xs.at[3])
    arrived(metar, ms.at[0])
    arrived(HX, fs.at[0])
    arrived(VX, fs.at[1])
    arrived(ebuf.at[pl.ds(0, 11)], es.at[0])
    for s in range(SWEEPS):
        arrived(SB.at[s], rss.at[s])
        arrived(SB.at[s], ags.at[s])
    for e in (0, 1):

        @pl.when(t + 1 < NT if e == 0 else t >= 1)
        def _():
            arrived(swaph.at[e], sws.at[0, e])
            arrived(swapv.at[e], sws.at[1, e])


def on_device(
    chains, weights, visible_bias, hidden_bias, inv_temps, hidden_thresholds, visible_thresholds, swap_phase, swap_accept
):
    vmem = pl.BlockSpec(memory_space=pltpu.VMEM)
    hbm = pl.BlockSpec(memory_space=pl.ANY)
    dma, mem = pltpu.SemaphoreType.DMA, pltpu.VMEM
    n = len(MSGS)
    vis, hid, energy = pl.pallas_call(
        kernel,
        out_shape=(mem((ROWS, BLK), BF16), mem((ROWS, BLK), BF16), mem((2, 128), F32)),
        in_specs=[hbm, hbm, vmem, vmem, vmem, hbm, hbm, vmem, vmem],
        out_specs=(vmem, vmem, vmem),
        scratch_shapes=[
            mem((2, 4096, BLK), BF16),
            mem((3, 16, HALF, CW), BF16),
            mem((4, HALF, CW), BF16),
            mem((4, 2, HALF, BLK), I32),
            mem((2, HALF, BLK), BF16),
            mem((2, HALF, BLK), BF16),
            mem((1, BLK), F32),
            mem((4, 2, HALF, BLK), F32),
            mem((2, HALF, BLK), F32),
            mem((16, HALF, CW), F32),
            mem((2, 2, HALF, BLK), BF16),
            mem((HALF, BLK), BF16),
            mem((4, HALF, CW), BF16),
            mem((2, 8, HALF, CW), BF16),
            mem((2, 8, HALF, CW), BF16),
            mem((8, 128), F32),
            mem((2, 8, 128), F32),
            mem((2, 2, 4, HALF, CW), BF16),
            mem((2, 2, HALF, BLK), BF16),
            mem((HALF, 128), F32),
            mem((ROWS, 128), F32),
            mem((ROWS, 128), F32),
            mem((12, 8, 128), F32),
            dma((2,)), dma((n,)), dma((2, 2)), dma((4,)), dma((5,)),
            dma((2,)), dma((2, 8)), dma((2,)), dma((2, 8)), dma((2,)), dma((5,)),
            dma((2, 2)), dma((2, 2)), dma((2,)), dma((2,)), dma((17,)),
        ],
        compiler_params=pltpu.CompilerParams(
            collective_id=0, has_side_effects=True, vmem_limit_bytes=58 * 2**20
        ),
        name="tempered",
    )(
        chains,
        weights,
        visible_bias.reshape(4, 1, BLK),
        hidden_bias.reshape(1, BLK),
        inv_temps.reshape(1, 1),
        hidden_thresholds,
        visible_thresholds,
        swap_phase.reshape(2, 128),
        swap_accept.reshape(2, 128),
    )
    return vis, hid, energy.reshape(ROWS)


def solution(mesh):
    return jax.shard_map(
        on_device,
        mesh=mesh,
        in_specs=(
            P("temp", "mp"),
            P("temp", "mp"),
            P(),
            P("mp"),
            P("temp"),
            P(None, "temp", "mp"),
            P(None, "temp", None),
            P(),
            P("temp"),
        ),
        out_specs=(P("temp", "mp"), P("temp", "mp"), P("temp")),
        check_vma=False,
    )
```

```python
import heapq

import jax
import jax.numpy as jnp
from jax import lax
from jax.experimental import pallas as pl
from jax.experimental.pallas import tpu as pltpu
from jax.sharding import PartitionSpec as P

NH = 4096
SWEEPS = 2
NY, NZ, NX, NT = 4, 8, 4, 64
ROWS, HALF, BLK, CW = 256, 128, 1024, 256
F32, BF16, I32 = jnp.float32, jnp.bfloat16, jnp.int32
MESH = pl.DeviceIdType.MESH
FIRST = (24, 32)


def gather_plan(p):
    na = FIRST[p]
    nb = 64 - na
    ha, hb = (na // 2 + 7) // 8 * 8, (nb // 2 + 7) // 8 * 8
    own = [] if p == 0 else [(1, "XW")]
    msgs = []

    def add(name, step, owner, first, rows, deps):
        msgs.append(((p, *name), step, owner, first, rows, [d if d in own else (p, *d) for d in deps] if deps else own))

    deepest = 4 - p
    for d in range(1, deepest + 1):
        for s in (1, -1):
            first, rows = (na, nb) if d < 4 else ((na, hb) if s > 0 else (na + hb, nb - hb))
            add(("BZ", s, d), (0, s), (0, -s * (d - 1)), first, rows, [("BZ", s, d - 1)] if d > 1 else [])
    add(("AY", 1, 1), (1, 0), (0, 0), 0, na, [])
    add(("AY", -1, 1), (-1, 0), (0, 0), 0, na, [])
    add(("AY", 1, 2), (1, 0), (-1, 0), 0, ha, [("AY", 1, 1)])
    add(("AY", -1, 2), (-1, 0), (1, 0), ha, na - ha, [("AY", -1, 1)])
    there = ([], [("AY", 1, 1)], [("AY", -1, 1)], [("AY", 1, 2), ("AY", -1, 2)])
    for d in range(1, deepest + 1):
        for j, oy in enumerate((0, -1, 1, 2)):
            for s in (1, -1):
                if d == 4 and (j < 2) != (s > 0):
                    continue
                deps = there[j] if d == 1 else [("AZ", s, d - 1, j)]
                add(("AZ", s, d, j), (0, s), (oy, -s * (d - 1)), 0, na, deps)
    for zz in (0, -1, 1, -2, 2, -3, 3, 4)[: 8 - p]:
        deps = [] if zz == 0 else ([("BZ", 1, 4), ("BZ", -1, 4)] if zz == 4 else [("BZ", -1 if zz > 0 else 1, abs(zz))])
        for s in (1, -1):
            add(("BY", s, 1, zz), (s, 0), (0, zz), na, nb, deps)
        s = 1 if zz in (0, 1, -2, 3) else -1
        add(("BY", s, 2, zz), (s, 0), (-s, zz), na, nb, [("BY", s, 1, zz)])
    if p == 1:
        whole = {
            0: [("AZ", 1, 4, 0), ("BZ", 1, 4), ("BZ", -1, 4)],
            -1: [("AZ", 1, 4, 1), ("BY", 1, 1, 4)],
            1: [("AZ", -1, 4, 2), ("BY", -1, 1, 4)],
            2: [("AZ", -1, 4, 3), ("BY", -1, 2, 4)],
        }
        for oy, deps in whole.items():
            msgs.append(((1, "XB", oy), None, (oy, 4), 0, 64, [(0, *d) for d in deps]))
    return msgs


def arrival_order(msgs):
    free, done, left = {None: 29.5}, set(), list(msgs)
    events, sends, waits = [(9.0, -1, (1, "XW"))], {}, []

    def issue(now):
        out = []
        for m in list(left):
            ahead = 3.0 if m[0][0] and any(o[0][0] == 0 and o[1] == m[1] for o in left) else 4.0
            if all(d in done for d in m[5]) and (m[1] is None or free.get(m[1], 0.0) - now < ahead):
                left.remove(m)
                begin = max(now, free.get(m[1], 0.0))
                free[m[1]] = begin + 1.4 * m[4] / 32
                heapq.heappush(events, (free[m[1]] + (2.2 if m[1] else 3.5), len(msgs) - len(left), m[0]))
                out.append(m[0])
        return out

    sends[None] = issue(0.0)
    while events:
        now, _, name = heapq.heappop(events)
        done.add(name)
        waits.append(name)
        sends[name] = issue(now)
    assert not left
    return sends, waits


MSGS = gather_plan(0) + gather_plan(1)
INDEX = {m[0]: i for i, m in enumerate(MSGS)}
SENDS, WAITS = arrival_order(MSGS)
LAST0 = max(n for n, name in enumerate(WAITS) if name[0] == 0)


def kernel(
    chains, weights, vbias, hbias, temps, hthr, vthr, phase, accept,
    vis_out, hid_out, energy_out,
    W, V, CO, thr, TS, TR, hbr, L, acc, PA, H, HX, VX, SB, RB, meta, metar, swapv, swaph, BT, TU, TL, ebuf,
    gs, gr, dsem, xs, xr, ags, agr, rss, rsr, fs, fr, sws, swr, ms, es, lsem,
):
    t = lax.axis_index("temp")
    m = lax.axis_index("mp")
    c = lax.rem(t, 2)
    z = lax.rem(t // 2, NZ)
    y = t // (2 * NZ)

    def col(d):
        return lax.rem(m + d + NX, NX)

    def rep(d):
        return lax.rem(t + d + NT, NT)

    def temp_of(dy, dz):
        return (lax.rem(y + dy + NY, NY) * NZ + lax.rem(z + dz + NZ, NZ)) * 2 + c

    step = 1 - 2 * lax.rem(m + c, 2)
    partner, other, far = (t, col(step)), (t, col(-step)), (t, col(2))
    a = lax.rem(m - c + NX, NX) // 2
    mine = pl.ds(pl.multiple_of(a * HALF, HALF), HALF)
    theirs = pl.ds(pl.multiple_of((1 - a) * HALF, HALF), HALF)

    def units(s, half, mate=False):
        if half:
            return col(step) if mate else m
        if s < SWEEPS - 1:
            return col(step + 2) if mate else col(2)
        return col(2) if mate else col(-step)

    def send(src, dst, ssem, rsem, device):
        copy = pltpu.make_async_remote_copy(
            src_ref=src, dst_ref=dst, send_sem=ssem, recv_sem=rsem, device_id=device, device_id_type=MESH
        )
        copy.start()

    def arrived(ref, sem):
        pltpu.make_async_copy(ref, ref, sem).wait()

    def load(src, dst, i):
        copy = pltpu.make_async_copy(src, dst, lsem.at[i])
        copy.start()
        return copy

    block = pl.ds(pl.multiple_of(t * 64, 64), 64)
    wload = load(weights, W.at[0, block], 0)
    vload = [load(chains.at[mine, pl.ds(j * CW, CW)], V.at[0, 4 * m + j], 1 + j) for j in range(4)]
    oload = [load(chains.at[theirs, pl.ds(j * CW, CW)], CO.at[j], 5 + j) for j in range(4)]
    tload = {}
    for s in range(SWEEPS):
        tload[2 * s, 1] = load(hthr.at[s, theirs], thr.at[2 * s, 1], 9 + 4 * s)
        tload[2 * s, 0] = load(hthr.at[s, mine], thr.at[2 * s, 0], 10 + 4 * s)
        for p in range(2):
            cols = pl.ds(pl.multiple_of(units(s, 1 - p) * BLK, BLK), BLK)
            tload[2 * s + 1, p] = load(vthr.at[s, mine, cols], thr.at[2 * s + 1, p], 11 + 4 * s + p)
    beta = temps[0:1, 0:1]
    meta[...] = jnp.broadcast_to(beta, (8, 128))
    meta[0:2, :] = accept[...].astype(F32)

    barrier = pltpu.get_barrier_semaphore()
    peers = [(t, col(1)), (t, col(-1)), (t, col(2)), (rep(1), m), (rep(-1), m)]
    peers += [(temp_of(1, 0), m), (temp_of(-1, 0), m), (temp_of(0, 1), m), (temp_of(0, -1), m)]
    for peer in peers:
        pl.semaphore_signal(barrier, inc=1, device_id=peer, device_id_type=MESH)
    pl.semaphore_wait(barrier, len(peers))

    sibling = (t + 1 - 2 * c, m)

    def place(name, seen):
        p = name[0]
        _, hop, (oy, oz), first, rows, _ = MSGS[INDEX[name]]
        sy, sz = hop or (0, 0)
        start = temp_of(oy - (sy if seen else 0), oz - (sz if seen else 0)) * 64 + first
        return W.at[p, pl.ds(pl.multiple_of(start, 8), rows)]

    def launch(name):
        i = INDEX[name]
        ref = place(name, False)
        if MSGS[i][1] is None:
            start = pl.multiple_of(temp_of(*MSGS[i][2]) * 64, 64)
            send(W.at[0, pl.ds(start, 64)], ref, gs.at[1], gr.at[i], far)
            return
        send(ref, ref, gs.at[name[0]], gr.at[i], (temp_of(*MSGS[i][1]), m))

    def to_sibling(p, ref):
        send(ref, ref, dsem.at[p, 0], dsem.at[p, 1], sibling)

    wload.wait()
    for name in SENDS[None]:
        launch(name)
    send(W.at[0, block], W.at[1, block], xs.at[0], xr.at[0], far)
    to_sibling(0, W.at[0, block])
    for cp in vload:
        cp.wait()
    own_v = V.at[0, pl.ds(4 * m, 4)]
    send(own_v, own_v, xs.at[1], xr.at[1], partner)
    for cp in oload:
        cp.wait()
    send(CO, own_v, xs.at[1], xr.at[1], other)
    send(CO, own_v, xs.at[1], xr.at[1], far)
    send(hbias, hbr, xs.at[2], xr.at[2], far)
    for e in (0, 1):
        send(meta, metar.at[e], ms.at[0], ms.at[1], (rep(1 - 2 * e), m))

    def send_thresholds(s):
        tload[2 * s, 1].wait()
        TS[s] = thr[2 * s, 1].astype(F32).astype(BF16)
        send(TS.at[s], TR.at[s], xs.at[3], xr.at[3 + s], far)

    def prepare(k, p):
        if k % 2 == 0 and p == 1:
            arrived(TR.at[k // 2], xr.at[3 + k // 2])
            if k == 0:
                arrived(hbr, xr.at[2])
        else:
            tload[k, p].wait()

        def some(i, carry):
            r = pl.ds(pl.multiple_of(i * 32, 32), 32)
            if k % 2 == 0 and p == 1:
                value, bias = TR[k // 2, r, :], hbr[...]
            else:
                value, bias = thr[k, p, r, :], (hbias[...] if k % 2 == 0 else vbias[units(k // 2, 1 - p)])
            level = (value.astype(F32) + 0.5) / 256.0
            L[k, p, r, :] = beta * bias + (jnp.log(level) - jnp.log(1.0 - level))
            return carry

        lax.fori_loop(0, HALF // 32, some, 0)

    def decisions():
        arrived(metar, ms.at[1])
        low, up = metar.at[0], metar.at[1]
        ph = phase[...]
        lower = (lax.rem(t, 2) == ph) & (t + 1 < NT)
        upper = (lax.rem(t + 1, 2) == ph) & (t >= 1)
        take_up = jnp.where(lower & (accept[...] == 1), 1.0, 0.0)
        take_low = jnp.where(upper & (low[0:2, :] > 0.5), 1.0, 0.0)
        b = jnp.where(take_up > 0.5, up[2:4, :], jnp.where(take_low > 0.5, low[2:4, :], jnp.broadcast_to(beta, (2, 128))))
        for h in (0, 1):
            for ref, rows in ((TU, take_up), (TL, take_low)):
                ref[128 * h : 128 * h + 128, :] = jnp.broadcast_to(rows[h : h + 1, :], (128, 128)).T
        BT[...] = jnp.broadcast_to(jnp.where(a == 0, b[0:1, :], b[1:2, :]), (128, 128)).T
        return take_up, take_low

    def dot(x, w):
        return jnp.dot(x, w, preferred_element_type=F32)

    def dot_t(x, w):
        return lax.dot_general(x, w, (((1,), (1,)), ((), ())), preferred_element_type=F32)

    def wrows(k):
        return pl.ds(pl.multiple_of(k * CW, CW), CW)

    def add_product(ph, p, chunks, fresh, tiles=range(4)):
        for n in tiles:
            cols = pl.ds(n * CW, CW)
            total = None
            for k in chunks:
                part = dot(V[ph, k], W[p, wrows(k), cols])
                total = part if total is None else total + part
            acc[p, :, cols] = total if fresh else acc[p, :, cols] + total

    def hidden_states(s, p):
        def tile(n, carry):
            cols = pl.ds(pl.multiple_of(n * CW, CW), CW)
            H[s, p, :, cols] = jax.nn.sigmoid(beta * acc[p, :, cols] + L[2 * s, p, :, cols]).astype(BF16)
            return carry

        lax.fori_loop(0, 4, tile, 0)

    def first_half():
        half0 = W.at[0, pl.ds(0, NT // 2 * 64)]
        arrived(half0, dsem.at[0, 1])
        arrived(V.at[0, pl.ds(0, 12)], xr.at[1])

    def first_partials(g):
        for k in (2 * g, 2 * g + 1):
            PA[k] = dot_t(H[0, 0], W[0, wrows(k), :])

    flags = None
    early = [lambda: send_thresholds(0), lambda: send_thresholds(1)]
    early += [lambda k=k, p=p: prepare(k, p) for k, p in ((0, 0), (1, 0), (1, 1), (2, 0), (3, 0), (3, 1))]
    late = [first_half] + [lambda n=n: add_product(0, 0, range(16), True, (n,)) for n in range(4)]
    late += [lambda: hidden_states(0, 0)] + [lambda g=g: first_partials(g) for g in range(8)]
    late += [lambda: prepare(0, 1), lambda: prepare(2, 1)]
    for n, name in enumerate(WAITS):
        if name[1] == "XW":
            ref = W.at[1, block]
            arrived(ref, xr.at[0])
        else:
            ref = place(name, True)
            arrived(ref, gr.at[INDEX[name]])
        for nxt in SENDS[name]:
            launch(nxt)
        to_sibling(name[0], ref)
        if n >= 4 and n % 3 == 0 and early:
            early.pop(0)()
        if n == 32:
            flags = decisions()
        if n >= LAST0 + 4 and late:
            late.pop(0)()
    for job in early + late:
        job()
    take_up, take_low = flags
    arrived(W.at[1, pl.ds(0, NT // 2 * 64)], dsem.at[1, 1])

    def partial(s, k):
        if s == 0:
            return PA[k] + dot_t(H[0, 1], W[1, wrows(k), :])
        return dot_t(H[s, 0], W[0, wrows(k), :]) + dot_t(H[s, 1], W[1, wrows(k), :])

    def visible_states(s):
        def give(i, term):
            SB[s, i] = term.astype(BF16)
            send(SB.at[s, i], RB.at[s, i], rss.at[s], rsr.at[s, i], partner)

        def keep(i, own):
            j, half = i % 4, i // 4
            k = 4 * units(s, half) + j
            arrived(RB.at[s, i], rsr.at[s, i])
            pre = own + RB[s, i].astype(F32)
            V[s + 1, k] = jax.nn.sigmoid(beta * pre + L[2 * s + 1, 1 - half, :, j * CW : j * CW + CW]).astype(BF16)
            ref = V.at[s + 1, k]
            send(ref, ref, ags.at[s], agr.at[s, i], partner)
            if s < SWEEPS - 1:
                return
            if half == 0:
                send(ref, VX.at[j], fs.at[1], fr.at[1 + j], other)
                return
            swap(ref, lambda e: swapv.at[e, a, j], 1)

        jobs = [(give, i, 4 * units(s, i // 4, True) + i % 4) for i in range(8)]
        jobs += [(keep, i, 4 * units(s, i // 4) + i % 4) for i in range(8)]
        def terms(n):
            return [partial(s, jobs[n + e][2]) for e in (0, 1)]

        ahead = terms(0)
        for n in range(0, len(jobs), 2):
            now, ahead = ahead, (terms(n + 2) if n + 2 < len(jobs) else None)
            for e in (0, 1):
                job, i, _ = jobs[n + e]
                job(i, now[e])

    def swap(src, dst, kind):
        for e in (0, 1):

            @pl.when(t + 1 < NT if e == 0 else t >= 1)
            def _():
                send(src, dst(e), sws.at[kind, e], swr.at[kind, e], (rep(1 - 2 * e), m))

    def gathered_product(ph):
        own = [4 * units(ph - 1, i // 4) + i % 4 for i in range(8)]
        if ph == SWEEPS:
            swap_far(0)
        add_product(ph, 0, own, True)
        if ph == SWEEPS:
            swap_far(1)
        add_product(ph, 1, own, True)
        for i in range(0, 8, 2):
            ks = [4 * units(ph - 1, i // 4, True) + i % 4 + e for e in (0, 1)]
            for e in (0, 1):
                arrived(V.at[ph, ks[e]], agr.at[ph - 1, i + e])
            for p in (0, 1):
                add_product(ph, p, ks, False)
            if ph == SWEEPS and i < 4:
                swap_far(2 + i // 2)

    def swap_far(j):
        arrived(VX.at[j], fr.at[1 + j])
        swap(VX.at[j], lambda e: swapv.at[e, 1 - a, j], 1)

    add_product(0, 1, range(16), True)
    hidden_states(0, 1)
    visible_states(0)
    gathered_product(1)
    for p in (1, 0):
        hidden_states(1, p)
    send(H.at[1, 1], HX, fs.at[0], fr.at[0], far)
    swap(H.at[1, 0], lambda e: swaph.at[e, a], 0)
    visible_states(1)
    arrived(HX, fr.at[0])
    swap(HX, lambda e: swaph.at[e, 1 - a], 0)

    def lanes(g):
        return pl.ds(pl.multiple_of(g * 128, 128), 128)

    total = jnp.zeros((HALF, 128), F32)
    for p in (0, 1):
        q = units(SWEEPS - 1, 1 - p)

        def bias_part(g, value):
            return value + V[2, 4 * q + g // 2, :, lanes(lax.rem(g, 2))].astype(F32) * vbias[q, :, lanes(g)]

        total = lax.fori_loop(0, 8, bias_part, total)
    total = BT[...] * total
    gathered_product(2)
    for p in (0, 1):
        bias_ref = hbr if p else hbias

        def soft_part(g, value):
            x = BT[...] * (acc[p, :, lanes(g)] + bias_ref[:, lanes(g)])
            return value + (jnp.maximum(x, 0.0) + jnp.log(1.0 + jnp.exp(-jnp.abs(x))))

        total = lax.fori_loop(0, 8, soft_part, total)
    ebuf[m] = jnp.broadcast_to(jnp.sum(total.T, axis=0, keepdims=True) * (-1.0 / NH), (8, 128))
    targets = [(0, d) for d in (1, 2, 3)] + [(e, d) for e in (1, -1) for d in range(4)]
    for e, d in targets:
        send(ebuf.at[m], ebuf.at[(e % 3) * NX + m], es.at[0], es.at[1], (rep(e), col(d)))

    def swapped(ref, kind):
        for e in (0, 1):
            there = t >= 1 if e == 0 else t + 1 < NT

            @pl.when(there)
            def _():
                arrived(ref.at[e], swr.at[kind, e])

            @pl.when(jnp.logical_not(there))
            def _():
                ref[e] = jnp.zeros(ref.shape[1:], BF16)

    swapped(swaph, 0)

    def chosen(rows, up, low, own):
        value = jnp.where(TL[rows, :] > 0.5, low.astype(F32), own.astype(F32))
        return jnp.where(TU[rows, :] > 0.5, up.astype(F32), value).astype(BF16)

    def swap_hidden(g, carry):
        cols = lanes(g)
        hid_out[mine, cols] = chosen(mine, swaph[1, a, :, cols], swaph[0, a, :, cols], H[1, 0, :, cols])
        hid_out[theirs, cols] = chosen(theirs, swaph[1, 1 - a, :, cols], swaph[0, 1 - a, :, cols], HX[:, cols])
        return carry

    lax.fori_loop(0, 8, swap_hidden, 0)
    swapped(swapv, 1)

    def swap_visible(g, carry):
        k, cols, out = g // 2, lanes(lax.rem(g, 2)), lanes(g)
        vis_out[mine, out] = chosen(mine, swapv[1, a, k, :, cols], swapv[0, a, k, :, cols], V[2, 4 * m + k, :, cols])
        vis_out[theirs, out] = chosen(theirs, swapv[1, 1 - a, k, :, cols], swapv[0, 1 - a, k, :, cols], VX[k, :, cols])
        return carry

    lax.fori_loop(0, 8, swap_visible, 0)
    arrived(ebuf.at[pl.ds(0, 11)], es.at[1])

    def summed(k):
        parity = c if k == 0 else 1 - c
        low = ebuf[k * NX + parity, 0:1, :] + ebuf[k * NX + parity + 1, 0:1, :]
        high = ebuf[k * NX + parity + 2, 0:1, :] + ebuf[k * NX + lax.rem(parity + 3, NX), 0:1, :]
        return low, high

    sums = [summed(k) for k in range(3)]
    for h in (0, 1):
        value = jnp.where(take_low[h : h + 1] > 0.5, sums[1][h], sums[0][h])
        energy_out[h : h + 1, :] = jnp.where(take_up[h : h + 1] > 0.5, sums[2][h], value)

    for p in (0, 1):
        arrived(W.at[p, pl.ds(0, 31 * 64)], gs.at[p])
        arrived(W.at[p, pl.ds(0, NT // 2 * 64)], dsem.at[p, 0])
    arrived(W.at[0, block], xs.at[0])
    arrived(V.at[0, pl.ds(0, 12)], xs.at[1])
    arrived(hbr, xs.at[2])
    arrived(TR, xs.at[3])
    arrived(metar, ms.at[0])
    arrived(HX, fs.at[0])
    arrived(VX, fs.at[1])
    arrived(ebuf.at[pl.ds(0, 11)], es.at[0])
    for s in range(SWEEPS):
        arrived(SB.at[s], rss.at[s])
        arrived(SB.at[s], ags.at[s])
    for e in (0, 1):

        @pl.when(t + 1 < NT if e == 0 else t >= 1)
        def _():
            arrived(swaph.at[e], sws.at[0, e])
            arrived(swapv.at[e], sws.at[1, e])


def on_device(
    chains, weights, visible_bias, hidden_bias, inv_temps, hidden_thresholds, visible_thresholds, swap_phase, swap_accept
):
    vmem = pl.BlockSpec(memory_space=pltpu.VMEM)
    hbm = pl.BlockSpec(memory_space=pl.ANY)
    dma, mem = pltpu.SemaphoreType.DMA, pltpu.VMEM
    n = len(MSGS)
    vis, hid, energy = pl.pallas_call(
        kernel,
        out_shape=(mem((ROWS, BLK), BF16), mem((ROWS, BLK), BF16), mem((2, 128), F32)),
        in_specs=[hbm, hbm, vmem, vmem, vmem, hbm, hbm, vmem, vmem],
        out_specs=(vmem, vmem, vmem),
        scratch_shapes=[
            mem((2, 4096, BLK), BF16),
            mem((3, 16, HALF, CW), BF16),
            mem((4, HALF, CW), BF16),
            mem((4, 2, HALF, BLK), I32),
            mem((2, HALF, BLK), BF16),
            mem((2, HALF, BLK), BF16),
            mem((1, BLK), F32),
            mem((4, 2, HALF, BLK), F32),
            mem((2, HALF, BLK), F32),
            mem((16, HALF, CW), F32),
            mem((2, 2, HALF, BLK), BF16),
            mem((HALF, BLK), BF16),
            mem((4, HALF, CW), BF16),
            mem((2, 8, HALF, CW), BF16),
            mem((2, 8, HALF, CW), BF16),
            mem((8, 128), F32),
            mem((2, 8, 128), F32),
            mem((2, 2, 4, HALF, CW), BF16),
            mem((2, 2, HALF, BLK), BF16),
            mem((HALF, 128), F32),
            mem((ROWS, 128), F32),
            mem((ROWS, 128), F32),
            mem((12, 8, 128), F32),
            dma((2,)), dma((n,)), dma((2, 2)), dma((4,)), dma((5,)),
            dma((2,)), dma((2, 8)), dma((2,)), dma((2, 8)), dma((2,)), dma((5,)),
            dma((2, 2)), dma((2, 2)), dma((2,)), dma((2,)), dma((17,)),
        ],
        compiler_params=pltpu.CompilerParams(
            collective_id=0, has_side_effects=True, vmem_limit_bytes=58 * 2**20
        ),
        name="tempered",
    )(
        chains,
        weights,
        visible_bias.reshape(4, 1, BLK),
        hidden_bias.reshape(1, BLK),
        inv_temps.reshape(1, 1),
        hidden_thresholds,
        visible_thresholds,
        swap_phase.reshape(2, 128),
        swap_accept.reshape(2, 128),
    )
    return vis, hid, energy.reshape(ROWS)


def solution(mesh):
    return jax.shard_map(
        on_device,
        mesh=mesh,
        in_specs=(
            P("temp", "mp"),
            P("temp", "mp"),
            P(),
            P("mp"),
            P("temp"),
            P(None, "temp", "mp"),
            P(None, "temp", None),
            P(),
            P("temp"),
        ),
        out_specs=(P("temp", "mp"), P("temp", "mp"), P("temp")),
        check_vma=False,
    )
```

```python
import heapq

import jax
import jax.numpy as jnp
from jax import lax
from jax.experimental import pallas as pl
from jax.experimental.pallas import tpu as pltpu
from jax.sharding import PartitionSpec as P

NH = 4096
SWEEPS = 2
NY, NZ, NX, NT = 4, 8, 4, 64
ROWS, HALF, BLK, CW = 256, 128, 1024, 256
F32, BF16, I32 = jnp.float32, jnp.bfloat16, jnp.int32
MESH = pl.DeviceIdType.MESH
HY_AT = 12
FIRST = (24, 32)


def gather_plan(p):
    na = FIRST[p]
    nb = 64 - na
    ha, hb = (na // 2 + 7) // 8 * 8, (nb // 2 + 7) // 8 * 8
    own = [] if p == 0 else [(1, "XW")]
    msgs = []

    def add(name, step, owner, first, rows, deps):
        msgs.append(((p, *name), step, owner, first, rows, [d if d in own else (p, *d) for d in deps] if deps else own))

    deepest = 4 - p
    for d in range(1, deepest + 1):
        for s in (1, -1):
            first, rows = (na, nb) if d < 4 else ((na, hb) if s > 0 else (na + hb, nb - hb))
            add(("BZ", s, d), (0, s), (0, -s * (d - 1)), first, rows, [("BZ", s, d - 1)] if d > 1 else [])
    add(("AY", 1, 1), (1, 0), (0, 0), 0, na, [])
    add(("AY", -1, 1), (-1, 0), (0, 0), 0, na, [])
    add(("AY", 1, 2), (1, 0), (-1, 0), 0, ha, [("AY", 1, 1)])
    add(("AY", -1, 2), (-1, 0), (1, 0), ha, na - ha, [("AY", -1, 1)])
    there = ([], [("AY", 1, 1)], [("AY", -1, 1)], [("AY", 1, 2), ("AY", -1, 2)])
    for d in range(1, deepest + 1):
        for j, oy in enumerate((0, -1, 1, 2)):
            for s in (1, -1):
                if d == 4 and (j < 2) != (s > 0):
                    continue
                deps = there[j] if d == 1 else [("AZ", s, d - 1, j)]
                add(("AZ", s, d, j), (0, s), (oy, -s * (d - 1)), 0, na, deps)
    for zz in (0, -1, 1, -2, 2, -3, 3, 4)[: 8 - p]:
        deps = [] if zz == 0 else ([("BZ", 1, 4), ("BZ", -1, 4)] if zz == 4 else [("BZ", -1 if zz > 0 else 1, abs(zz))])
        for s in (1, -1):
            add(("BY", s, 1, zz), (s, 0), (0, zz), na, nb, deps)
        s = 1 if zz in (0, 1, -2, 3) else -1
        add(("BY", s, 2, zz), (s, 0), (-s, zz), na, nb, [("BY", s, 1, zz)])
    if p == 1:
        whole = {
            0: [("AZ", 1, 4, 0), ("BZ", 1, 4), ("BZ", -1, 4)],
            -1: [("AZ", 1, 4, 1), ("BY", 1, 1, 4)],
            1: [("AZ", -1, 4, 2), ("BY", -1, 1, 4)],
            2: [("AZ", -1, 4, 3), ("BY", -1, 2, 4)],
        }
        for oy, deps in whole.items():
            msgs.append(((1, "XB", oy), None, (oy, 4), 0, 64, [(0, *d) for d in deps]))
    return msgs


def hop(name):
    return (*name[:2], *name[3:]) if name[1] in ("AY", "AZ", "BZ", "BY") else name


def arrival_order(msgs):
    free, done, left = {None: 29.5}, set(), list(msgs)
    events, sends, waits, due = [(9.0, -1, (1, "XW"))], {}, [], {}
    for m in msgs:
        due.setdefault(hop(m[0]), []).append(m[0])

    def issue(now):
        out = []
        for m in list(left):
            ahead = 3.0 if m[0][0] and any(o[0][0] == 0 and o[1] == m[1] for o in left) else 4.0
            if all(d in ready for d in m[5]) and (m[1] is None or free.get(m[1], 0.0) - now < ahead):
                left.remove(m)
                begin = max(now, free.get(m[1], 0.0))
                free[m[1]] = begin + 1.4 * m[4] / 32
                heapq.heappush(events, (free[m[1]] + (2.2 if m[1] else 3.5), len(msgs) - len(left), m[0]))
                out.append(m[0])
        return out

    ready = set()
    sends[None] = issue(0.0)
    while events:
        now, _, name = heapq.heappop(events)
        both = due.get(hop(name), [name])
        done.add(name)
        if all(other in done for other in both):
            ready.update(both)
            waits.append(both)
            sends[hop(name)] = issue(now)
    assert not left
    return sends, waits


MSGS = gather_plan(0) + gather_plan(1)
INDEX = {m[0]: i for i, m in enumerate(MSGS)}
SEMS = {h: i for i, h in enumerate(dict.fromkeys(hop(m[0]) for m in MSGS))}
SENDS, WAITS = arrival_order(MSGS)
LAST0 = max(n for n, names in enumerate(WAITS) if names[0][0] == 0)


def kernel(
    chains, weights, vbias_in, hbias_in, temps_in, hthr, vthr, phase_in, accept_in,
    vis_out, hid_out, energy_out,
    W, V, CO, thr, TS, TR, hbr, L, acc, PA, H, HX, VX, SB, RB, meta, metar, swapv, swaph, BT, TU, TL, ebuf, vbias, hbias, temps, phase, accept,
    gs, gr, dsem, xs, xr, ags, agr, rss, rsr, fs, fr, sws, swr, ms, es, lsem,
):
    t = lax.axis_index("temp")
    m = lax.axis_index("mp")
    c = lax.rem(t, 2)
    z = lax.rem(t // 2, NZ)
    y = t // (2 * NZ)

    def col(d):
        return lax.rem(m + d + NX, NX)

    def rep(d):
        return lax.rem(t + d + NT, NT)

    def temp_of(dy, dz):
        return (lax.rem(y + dy + NY, NY) * NZ + lax.rem(z + dz + NZ, NZ)) * 2 + c

    step = 1 - 2 * lax.rem(m + c, 2)
    partner, other, far = (t, col(step)), (t, col(-step)), (t, col(2))
    a = lax.rem(m - c + NX, NX) // 2
    mine = pl.ds(pl.multiple_of(a * HALF, HALF), HALF)
    theirs = pl.ds(pl.multiple_of((1 - a) * HALF, HALF), HALF)

    def units(s, half, mate=False):
        if half:
            return col(step) if mate else m
        if s < SWEEPS - 1:
            return col(step + 2) if mate else col(2)
        return col(2) if mate else col(-step)

    def send(src, dst, ssem, rsem, device):
        copy = pltpu.make_async_remote_copy(
            src_ref=src, dst_ref=dst, send_sem=ssem, recv_sem=rsem, device_id=device, device_id_type=MESH
        )
        copy.start()

    def arrived(ref, sem):
        pltpu.make_async_copy(ref, ref, sem).wait()

    def load(src, dst, i):
        copy = pltpu.make_async_copy(src, dst, lsem.at[i])
        copy.start()
        return copy

    block = pl.ds(pl.multiple_of(t * 64, 64), 64)
    wload = load(weights, W.at[0, block], 0)
    vload = [load(chains.at[mine, pl.ds(j * CW, CW)], V.at[0, 4 * m + j], 1 + j) for j in range(4)]
    oload = [load(chains.at[theirs, pl.ds(j * CW, CW)], CO.at[j], 5 + j) for j in range(4)]
    tload = {}
    for s in range(SWEEPS):
        tload[2 * s, 1] = load(hthr.at[s, theirs], thr.at[2 * s, 1], 9 + 4 * s)
        tload[2 * s, 0] = load(hthr.at[s, mine], thr.at[2 * s, 0], 10 + 4 * s)
        for p in range(2):
            cols = pl.ds(pl.multiple_of(units(s, 1 - p) * BLK, BLK), BLK)
            tload[2 * s + 1, p] = load(vthr.at[s, mine, cols], thr.at[2 * s + 1, p], 11 + 4 * s + p)
    small = [
        pltpu.make_async_copy(src, dst, lsem.at[17 + i])
        for i, (src, dst) in enumerate(((vbias_in, vbias), (hbias_in, hbias), (temps_in, temps), (phase_in, phase), (accept_in, accept)))
    ]
    for copy in small:
        copy.start()

    barrier = pltpu.get_barrier_semaphore()
    peers = [(t, col(1)), (t, col(-1)), (t, col(2)), (rep(1), m), (rep(-1), m)]
    peers += [(temp_of(1, 0), m), (temp_of(-1, 0), m), (temp_of(0, 1), m), (temp_of(0, -1), m)]
    for peer in peers:
        pl.semaphore_signal(barrier, inc=1, device_id=peer, device_id_type=MESH)
    pl.semaphore_wait(barrier, len(peers))

    for copy in small:
        copy.wait()
    beta = temps[0]
    meta[...] = jnp.full((8, 128), beta, F32)
    meta[0:2, :] = accept[...].astype(F32)

    sibling = (t + 1 - 2 * c, m)

    def place(name, seen):
        p = name[0]
        _, hop, (oy, oz), first, rows, _ = MSGS[INDEX[name]]
        sy, sz = hop or (0, 0)
        start = temp_of(oy - (sy if seen else 0), oz - (sz if seen else 0)) * 64 + first
        return W.at[p, pl.ds(pl.multiple_of(start, 8), rows)]

    def launch(name):
        i = INDEX[name]
        ref = place(name, False)
        if MSGS[i][1] is None:
            start = pl.multiple_of(temp_of(*MSGS[i][2]) * 64, 64)
            send(W.at[0, pl.ds(start, 64)], ref, gs.at[1], gr.at[SEMS[hop(name)]], far)
            return
        send(ref, ref, gs.at[name[0]], gr.at[SEMS[hop(name)]], (temp_of(*MSGS[i][1]), m))

    def to_sibling(p, ref):
        send(ref, ref, dsem.at[p, 0], dsem.at[p, 1], sibling)

    wload.wait()
    for name in SENDS[None]:
        launch(name)
    send(W.at[0, block], W.at[1, block], xs.at[0], xr.at[0], far)
    to_sibling(0, W.at[0, block])
    for cp in vload:
        cp.wait()
    own_v = V.at[0, pl.ds(4 * m, 4)]
    send(own_v, own_v, xs.at[1], xr.at[1], partner)
    for cp in oload:
        cp.wait()
    send(CO, own_v, xs.at[1], xr.at[1], other)
    send(CO, own_v, xs.at[1], xr.at[1], far)
    send(hbias, hbr, xs.at[2], xr.at[2], far)
    for e in (0, 1):
        send(meta, metar.at[e], ms.at[0], ms.at[1], (rep(1 - 2 * e), m))

    def send_thresholds(s):
        tload[2 * s, 1].wait()
        TS[s] = thr[2 * s, 1].astype(F32).astype(BF16)
        send(TS.at[s], TR.at[s], xs.at[3], xr.at[3 + s], far)

    def prepare(k, p):
        if k % 2 == 0 and p == 1:
            arrived(TR.at[k // 2], xr.at[3 + k // 2])
            if k == 0:
                arrived(hbr, xr.at[2])
        else:
            tload[k, p].wait()

        def some(i, carry):
            r = pl.ds(pl.multiple_of(i * 32, 32), 32)
            if k % 2 == 0 and p == 1:
                value, bias = TR[k // 2, r, :], hbr[...]
            else:
                value, bias = thr[k, p, r, :], (hbias[...] if k % 2 == 0 else vbias[units(k // 2, 1 - p)])
            level = (value.astype(F32) + 0.5) / 256.0
            L[k, p, r, :] = beta * bias + (jnp.log(level) - jnp.log(1.0 - level))
            return carry

        lax.fori_loop(0, HALF // 32, some, 0)

    def decisions():
        arrived(metar, ms.at[1])
        low, up = metar.at[0], metar.at[1]
        ph = phase[...]
        lower = (lax.rem(t, 2) == ph) & (t + 1 < NT)
        upper = (lax.rem(t + 1, 2) == ph) & (t >= 1)
        take_up = jnp.where(lower & (accept[...] == 1), 1.0, 0.0)
        take_low = jnp.where(upper & (low[0:2, :] > 0.5), 1.0, 0.0)
        b = jnp.where(take_up > 0.5, up[2:4, :], jnp.where(take_low > 0.5, low[2:4, :], jnp.full((2, 128), beta, F32)))
        for h in (0, 1):
            for ref, rows in ((TU, take_up), (TL, take_low)):
                ref[128 * h : 128 * h + 128, :] = jnp.broadcast_to(rows[h : h + 1, :], (128, 128)).T
        BT[...] = jnp.broadcast_to(jnp.where(a == 0, b[0:1, :], b[1:2, :]), (128, 128)).T
        return take_up, take_low

    def dot(x, w):
        return jnp.dot(x, w, preferred_element_type=F32)

    def dot_t(x, w):
        return lax.dot_general(x, w, (((1,), (1,)), ((), ())), preferred_element_type=F32)

    def wrows(k):
        return pl.ds(pl.multiple_of(k * CW, CW), CW)

    def add_product(ph, p, chunks, fresh, tiles=range(4)):
        for n in tiles:
            cols = pl.ds(n * CW, CW)
            total = None
            for k in chunks:
                part = dot(V[ph, k], W[p, wrows(k), cols])
                total = part if total is None else total + part
            acc[p, :, cols] = total if fresh else acc[p, :, cols] + total

    def hidden_states(s, p):
        def tile(n, carry):
            cols = pl.ds(pl.multiple_of(n * CW, CW), CW)
            H[s, p, :, cols] = jax.nn.sigmoid(beta * acc[p, :, cols] + L[2 * s, p, :, cols]).astype(BF16)
            return carry

        lax.fori_loop(0, 4, tile, 0)

    def first_half():
        half0 = W.at[0, pl.ds(0, NT // 2 * 64)]
        arrived(half0, dsem.at[0, 1])
        arrived(V.at[0, pl.ds(0, 12)], xr.at[1])

    def first_partials(g):
        for k in (2 * g, 2 * g + 1):
            PA[k] = dot_t(H[0, 0], W[0, wrows(k), :])

    flags = None
    early = [lambda: send_thresholds(0), lambda: send_thresholds(1)]
    early += [lambda k=k, p=p: prepare(k, p) for k, p in ((0, 0), (1, 0), (1, 1), (2, 0), (3, 0), (3, 1))]
    late = [first_half] + [lambda n=n: add_product(0, 0, range(16), True, (n,)) for n in range(4)]
    late += [lambda: hidden_states(0, 0)] + [lambda g=g: first_partials(g) for g in range(8)]
    late += [lambda: prepare(0, 1), lambda: prepare(2, 1)]
    for n, names in enumerate(WAITS):
        p = names[0][0]
        if names[0][1] == "XW":
            refs = [W.at[1, block]]
            arrived(refs[0], xr.at[0])
        else:
            refs = [place(name, True) for name in names]
            total = sum(MSGS[INDEX[name]][4] for name in names)
            arrived(W.at[p, pl.ds(0, total)], gr.at[SEMS[hop(names[0])]])
        for nxt in SENDS[hop(names[0])]:
            launch(nxt)
        for ref in refs:
            to_sibling(p, ref)
        if n >= 3 and n % 2 == 0 and early:
            early.pop(0)()
        if n == 18:
            flags = decisions()
        for _ in range(2):
            if n >= LAST0 + 2 and late:
                late.pop(0)()
    for job in early + late:
        job()
    take_up, take_low = flags
    arrived(W.at[1, pl.ds(0, NT // 2 * 64)], dsem.at[1, 1])

    def partial(s, k):
        if s == 0:
            return PA[k] + dot_t(H[0, 1], W[1, wrows(k), :])
        return dot_t(H[s, 0], W[0, wrows(k), :]) + dot_t(H[s, 1], W[1, wrows(k), :])

    def visible_states(s):
        def give(i, term):
            SB[s, i] = term.astype(BF16)
            send(SB.at[s, i], RB.at[s, i], rss.at[s], rsr.at[s, i], partner)

        def keep(i, own):
            j, half = i % 4, i // 4
            k = 4 * units(s, half) + j
            arrived(RB.at[s, i], rsr.at[s, i])
            pre = own + RB[s, i].astype(F32)
            V[s + 1, k] = jax.nn.sigmoid(beta * pre + L[2 * s + 1, 1 - half, :, j * CW : j * CW + CW]).astype(BF16)
            ref = V.at[s + 1, k]
            send(ref, ref, ags.at[s], agr.at[s, i], partner)
            if s < SWEEPS - 1:
                return
            if half == 0:
                send(ref, VX.at[j], fs.at[1], fr.at[1 + j], other)
                return
            swap(ref, lambda e: swapv.at[e, a, j], 1)

        jobs = [(give, i, 4 * units(s, i // 4, True) + i % 4) for i in range(8)]
        jobs += [(keep, i, 4 * units(s, i // 4) + i % 4) for i in range(8)]
        def terms(n):
            return [partial(s, jobs[n + e][2]) for e in (0, 1)]

        ahead = terms(0)
        for n in range(0, len(jobs), 2):
            now, ahead = ahead, (terms(n + 2) if n + 2 < len(jobs) else None)
            for e in (0, 1):
                job, i, _ = jobs[n + e]
                job(i, now[e])
            if s == SWEEPS - 1 and n == HY_AT:
                arrived(HX, fr.at[0])
                swap(HX, lambda e: swaph.at[e, 1 - a], 0)

    def swap(src, dst, kind):
        for e in (0, 1):

            @pl.when(t + 1 < NT if e == 0 else t >= 1)
            def _():
                send(src, dst(e), sws.at[kind, e], swr.at[kind, e], (rep(1 - 2 * e), m))

    def gathered_product(ph):
        own = [4 * units(ph - 1, i // 4) + i % 4 for i in range(8)]
        if ph == SWEEPS:
            swap_far(0)
        add_product(ph, 0, own, True)
        if ph == SWEEPS:
            swap_far(1)
        add_product(ph, 1, own, True)
        for i in range(0, 8, 2):
            ks = [4 * units(ph - 1, i // 4, True) + i % 4 + e for e in (0, 1)]
            for e in (0, 1):
                arrived(V.at[ph, ks[e]], agr.at[ph - 1, i + e])
            for p in (0, 1):
                add_product(ph, p, ks, False)
            if ph == SWEEPS and i < 4:
                swap_far(2 + i // 2)

    def swap_far(j):
        arrived(VX.at[j], fr.at[1 + j])
        swap(VX.at[j], lambda e: swapv.at[e, 1 - a, j], 1)

    add_product(0, 1, range(16), True)
    hidden_states(0, 1)
    visible_states(0)
    gathered_product(1)
    for p in (1, 0):
        hidden_states(1, p)
    send(H.at[1, 1], HX, fs.at[0], fr.at[0], far)
    swap(H.at[1, 0], lambda e: swaph.at[e, a], 0)
    visible_states(1)

    def lanes(g):
        return pl.ds(pl.multiple_of(g * 128, 128), 128)

    total = jnp.zeros((HALF, 128), F32)
    for p in (0, 1):
        q = units(SWEEPS - 1, 1 - p)

        def bias_part(g, value):
            return value + V[2, 4 * q + g // 2, :, lanes(lax.rem(g, 2))].astype(F32) * vbias[q, :, lanes(g)]

        total = lax.fori_loop(0, 8, bias_part, total)
    total = BT[...] * total
    gathered_product(2)
    for p in (0, 1):
        bias_ref = hbr if p else hbias

        def soft_part(g, value):
            x = BT[...] * (acc[p, :, lanes(g)] + bias_ref[:, lanes(g)])
            return value + (jnp.maximum(x, 0.0) + jnp.log(1.0 + jnp.exp(-jnp.abs(x))))

        total = lax.fori_loop(0, 8, soft_part, total)
    ebuf[m] = jnp.broadcast_to(jnp.sum(total.T, axis=0, keepdims=True) * (-1.0 / NH), (8, 128))
    targets = [(0, d) for d in (1, 2, 3)] + [(e, d) for e in (1, -1) for d in range(4)]
    for e, d in targets:
        send(ebuf.at[m], ebuf.at[(e % 3) * NX + m], es.at[0], es.at[1], (rep(e), col(d)))

    def swapped(ref, kind):
        for e in (0, 1):
            there = t >= 1 if e == 0 else t + 1 < NT

            @pl.when(there)
            def _():
                arrived(ref.at[e], swr.at[kind, e])

            @pl.when(jnp.logical_not(there))
            def _():
                ref[e] = jnp.zeros(ref.shape[1:], BF16)

    swapped(swaph, 0)

    def chosen(rows, up, low, own):
        value = jnp.where(TL[rows, :] > 0.5, low.astype(F32), own.astype(F32))
        return jnp.where(TU[rows, :] > 0.5, up.astype(F32), value).astype(BF16)

    def swap_hidden(g, carry):
        cols = lanes(g)
        hid_out[mine, cols] = chosen(mine, swaph[1, a, :, cols], swaph[0, a, :, cols], H[1, 0, :, cols])
        hid_out[theirs, cols] = chosen(theirs, swaph[1, 1 - a, :, cols], swaph[0, 1 - a, :, cols], HX[:, cols])
        return carry

    lax.fori_loop(0, 8, swap_hidden, 0)
    swapped(swapv, 1)

    def swap_visible(g, carry):
        k, cols, out = g // 2, lanes(lax.rem(g, 2)), lanes(g)
        vis_out[mine, out] = chosen(mine, swapv[1, a, k, :, cols], swapv[0, a, k, :, cols], V[2, 4 * m + k, :, cols])
        vis_out[theirs, out] = chosen(theirs, swapv[1, 1 - a, k, :, cols], swapv[0, 1 - a, k, :, cols], VX[k, :, cols])
        return carry

    lax.fori_loop(0, 8, swap_visible, 0)
    arrived(ebuf.at[pl.ds(0, 11)], es.at[1])

    def summed(k):
        parity = c if k == 0 else 1 - c
        low = ebuf[k * NX + parity, 0:1, :] + ebuf[k * NX + parity + 1, 0:1, :]
        high = ebuf[k * NX + parity + 2, 0:1, :] + ebuf[k * NX + lax.rem(parity + 3, NX), 0:1, :]
        return low, high

    sums = [summed(k) for k in range(3)]
    for h in (0, 1):
        value = jnp.where(take_low[h : h + 1] > 0.5, sums[1][h], sums[0][h])
        energy_out[h : h + 1, :] = jnp.where(take_up[h : h + 1] > 0.5, sums[2][h], value)

    for p in (0, 1):
        arrived(W.at[p, pl.ds(0, 31 * 64)], gs.at[p])
        arrived(W.at[p, pl.ds(0, NT // 2 * 64)], dsem.at[p, 0])
    arrived(W.at[0, block], xs.at[0])
    arrived(V.at[0, pl.ds(0, 12)], xs.at[1])
    arrived(hbr, xs.at[2])
    arrived(TR, xs.at[3])
    arrived(metar, ms.at[0])
    arrived(HX, fs.at[0])
    arrived(VX, fs.at[1])
    arrived(ebuf.at[pl.ds(0, 11)], es.at[0])
    for s in range(SWEEPS):
        arrived(SB.at[s], rss.at[s])
        arrived(SB.at[s], ags.at[s])
    for e in (0, 1):

        @pl.when(t + 1 < NT if e == 0 else t >= 1)
        def _():
            arrived(swaph.at[e], sws.at[0, e])
            arrived(swapv.at[e], sws.at[1, e])


def on_device(
    chains, weights, visible_bias, hidden_bias, inv_temps, hidden_thresholds, visible_thresholds, swap_phase, swap_accept
):
    vmem = pl.BlockSpec(memory_space=pltpu.VMEM)
    hbm = pl.BlockSpec(memory_space=pl.ANY)
    dma, mem = pltpu.SemaphoreType.DMA, pltpu.VMEM
    n = len(SEMS)
    vis, hid, energy = pl.pallas_call(
        kernel,
        out_shape=(mem((ROWS, BLK), BF16), mem((ROWS, BLK), BF16), mem((2, 128), F32)),
        in_specs=[hbm] * 9,
        out_specs=(vmem, vmem, vmem),
        scratch_shapes=[
            mem((2, 4096, BLK), BF16),
            mem((3, 16, HALF, CW), BF16),
            mem((4, HALF, CW), BF16),
            mem((4, 2, HALF, BLK), I32),
            mem((2, HALF, BLK), BF16),
            mem((2, HALF, BLK), BF16),
            mem((1, BLK), F32),
            mem((4, 2, HALF, BLK), F32),
            mem((2, HALF, BLK), F32),
            mem((16, HALF, CW), F32),
            mem((2, 2, HALF, BLK), BF16),
            mem((HALF, BLK), BF16),
            mem((4, HALF, CW), BF16),
            mem((2, 8, HALF, CW), BF16),
            mem((2, 8, HALF, CW), BF16),
            mem((8, 128), F32),
            mem((2, 8, 128), F32),
            mem((2, 2, 4, HALF, CW), BF16),
            mem((2, 2, HALF, BLK), BF16),
            mem((HALF, 128), F32),
            mem((ROWS, 128), F32),
            mem((ROWS, 128), F32),
            mem((12, 8, 128), F32),
            mem((4, 1, BLK), F32), mem((1, BLK), F32), pltpu.SMEM((1,), F32), mem((2, 128), I32), mem((2, 128), I32),
            dma((2,)), dma((n,)), dma((2, 2)), dma((4,)), dma((5,)),
            dma((2,)), dma((2, 8)), dma((2,)), dma((2, 8)), dma((2,)), dma((5,)),
            dma((2, 2)), dma((2, 2)), dma((2,)), dma((2,)), dma((22,)),
        ],
        compiler_params=pltpu.CompilerParams(
            collective_id=0, has_side_effects=True, vmem_limit_bytes=58 * 2**20
        ),
        name="tempered",
    )(
        chains,
        weights,
        visible_bias.reshape(4, 1, BLK),
        hidden_bias.reshape(1, BLK),
        inv_temps,
        hidden_thresholds,
        visible_thresholds,
        swap_phase.reshape(2, 128),
        swap_accept.reshape(2, 128),
    )
    return vis, hid, energy.reshape(ROWS)


def solution(mesh):
    return jax.shard_map(
        on_device,
        mesh=mesh,
        in_specs=(
            P("temp", "mp"),
            P("temp", "mp"),
            P(),
            P("mp"),
            P("temp"),
            P(None, "temp", "mp"),
            P(None, "temp", None),
            P(),
            P("temp"),
        ),
        out_specs=(P("temp", "mp"), P("temp", "mp"), P("temp")),
        check_vma=False,
    )
```

```python
import heapq

import jax
import jax.numpy as jnp
from jax import lax
from jax.experimental import pallas as pl
from jax.experimental.pallas import tpu as pltpu
from jax.sharding import PartitionSpec as P

NH = 4096
SWEEPS = 2
NY, NZ, NX, NT = 4, 8, 4, 64
ROWS, HALF, BLK, CW = 256, 128, 1024, 256
F32, BF16, I32 = jnp.float32, jnp.bfloat16, jnp.int32
MESH = pl.DeviceIdType.MESH
START = 4
HY_AT = 12
FIRST = (24, 32)


def gather_plan(p):
    na = FIRST[p]
    nb = 64 - na
    ha, hb = (na // 2 + 7) // 8 * 8, (nb // 2 + 7) // 8 * 8
    own = [] if p == 0 else [(1, "XW")]
    msgs = []

    def add(name, step, owner, first, rows, deps):
        msgs.append(((p, *name), step, owner, first, rows, [d if d in own else (p, *d) for d in deps] if deps else own))

    deepest = 4 - p
    for d in range(1, deepest + 1):
        for s in (1, -1):
            first, rows = (na, nb) if d < 4 else ((na, hb) if s > 0 else (na + hb, nb - hb))
            add(("BZ", s, d), (0, s), (0, -s * (d - 1)), first, rows, [("BZ", s, d - 1)] if d > 1 else [])
    add(("AY", 1, 1), (1, 0), (0, 0), 0, na, [])
    add(("AY", -1, 1), (-1, 0), (0, 0), 0, na, [])
    add(("AY", 1, 2), (1, 0), (-1, 0), 0, ha, [("AY", 1, 1)])
    add(("AY", -1, 2), (-1, 0), (1, 0), ha, na - ha, [("AY", -1, 1)])
    there = ([], [("AY", 1, 1)], [("AY", -1, 1)], [("AY", 1, 2), ("AY", -1, 2)])
    for d in range(1, deepest + 1):
        for j, oy in enumerate((0, -1, 1, 2)):
            for s in (1, -1):
                if d == 4 and (j < 2) != (s > 0):
                    continue
                deps = there[j] if d == 1 else [("AZ", s, d - 1, j)]
                add(("AZ", s, d, j), (0, s), (oy, -s * (d - 1)), 0, na, deps)
    for zz in (0, -1, 1, -2, 2, -3, 3, 4)[: 8 - p]:
        deps = [] if zz == 0 else ([("BZ", 1, 4), ("BZ", -1, 4)] if zz == 4 else [("BZ", -1 if zz > 0 else 1, abs(zz))])
        for s in (1, -1):
            add(("BY", s, 1, zz), (s, 0), (0, zz), na, nb, deps)
        s = 1 if zz in (0, 1, -2, 3) else -1
        add(("BY", s, 2, zz), (s, 0), (-s, zz), na, nb, [("BY", s, 1, zz)])
    if p == 1:
        whole = {
            0: [("AZ", 1, 4, 0), ("BZ", 1, 4), ("BZ", -1, 4)],
            -1: [("AZ", 1, 4, 1), ("BY", 1, 1, 4)],
            1: [("AZ", -1, 4, 2), ("BY", -1, 1, 4)],
            2: [("AZ", -1, 4, 3), ("BY", -1, 2, 4)],
        }
        for oy, deps in whole.items():
            msgs.append(((1, "XB", oy), None, (oy, 4), 0, 64, [(0, *d) for d in deps]))
    return msgs


def hop(name):
    return (*name[:2], *name[3:]) if name[1] in ("AY", "AZ", "BZ", "BY") else name


def arrival_order(msgs):
    free, done, left = {None: 29.5}, set(), list(msgs)
    events, sends, waits, due = [(9.0, -1, (1, "XW"))], {}, [], {}
    for m in msgs:
        due.setdefault(hop(m[0]), []).append(m[0])

    def issue(now):
        out = []
        for m in list(left):
            ahead = 3.0 if m[0][0] and any(o[0][0] == 0 and o[1] == m[1] for o in left) else 4.0
            if all(d in ready for d in m[5]) and (m[1] is None or free.get(m[1], 0.0) - now < ahead):
                left.remove(m)
                begin = max(now, free.get(m[1], 0.0))
                free[m[1]] = begin + 1.4 * m[4] / 32
                heapq.heappush(events, (free[m[1]] + (2.2 if m[1] else 3.5), len(msgs) - len(left), m[0]))
                out.append(m[0])
        return out

    ready = set()
    sends[None] = issue(0.0)
    while events:
        now, _, name = heapq.heappop(events)
        both = due.get(hop(name), [name])
        done.add(name)
        if all(other in done for other in both):
            ready.update(both)
            waits.append(both)
            sends[hop(name)] = issue(now)
    assert not left
    return sends, waits


MSGS = gather_plan(0) + gather_plan(1)
INDEX = {m[0]: i for i, m in enumerate(MSGS)}
SEMS = {h: i for i, h in enumerate(dict.fromkeys(hop(m[0]) for m in MSGS))}
SENDS, WAITS = arrival_order(MSGS)
LAST0 = max(n for n, names in enumerate(WAITS) if names[0][0] == 0)


def kernel(
    chains, weights, vbias_in, hbias_in, temps_in, hthr, vthr, phase_in, accept_in,
    vis_out, hid_out, energy_out,
    W, V, CO, thr, TS, TR, hbr, L, acc, PA, H, HX, VX, SB, RB, meta, metar, swapv, swaph, BT, TU, TL, ebuf, vbias, hbias, temps, phase, accept,
    gs, gr, dsem, xs, xr, ags, agr, rss, rsr, fs, fr, sws, swr, ms, es, lsem,
):
    t = lax.axis_index("temp")
    m = lax.axis_index("mp")
    c = lax.rem(t, 2)
    z = lax.rem(t // 2, NZ)
    y = t // (2 * NZ)

    def col(d):
        return lax.rem(m + d + NX, NX)

    def rep(d):
        return lax.rem(t + d + NT, NT)

    def temp_of(dy, dz):
        return (lax.rem(y + dy + NY, NY) * NZ + lax.rem(z + dz + NZ, NZ)) * 2 + c

    step = 1 - 2 * lax.rem(m + c, 2)
    partner, other, far = (t, col(step)), (t, col(-step)), (t, col(2))
    a = lax.rem(m - c + NX, NX) // 2
    mine = pl.ds(pl.multiple_of(a * HALF, HALF), HALF)
    theirs = pl.ds(pl.multiple_of((1 - a) * HALF, HALF), HALF)

    def units(s, half, mate=False):
        if half:
            return col(step) if mate else m
        if s < SWEEPS - 1:
            return col(step + 2) if mate else col(2)
        return col(2) if mate else col(-step)

    def send(src, dst, ssem, rsem, device):
        copy = pltpu.make_async_remote_copy(
            src_ref=src, dst_ref=dst, send_sem=ssem, recv_sem=rsem, device_id=device, device_id_type=MESH
        )
        copy.start()

    def arrived(ref, sem):
        pltpu.make_async_copy(ref, ref, sem).wait()

    def load(src, dst, i):
        copy = pltpu.make_async_copy(src, dst, lsem.at[i])
        copy.start()
        return copy

    block = pl.ds(pl.multiple_of(t * 64, 64), 64)
    wload = load(weights, W.at[0, block], 0)
    vload = [load(chains.at[mine, pl.ds(j * CW, CW)], V.at[0, 4 * m + j], 1 + j) for j in range(4)]
    oload = [load(chains.at[theirs, pl.ds(j * CW, CW)], CO.at[j], 5 + j) for j in range(4)]
    tload = {}
    for s in range(SWEEPS):
        tload[2 * s, 1] = load(hthr.at[s, theirs], thr.at[2 * s, 1], 9 + 4 * s)
        tload[2 * s, 0] = load(hthr.at[s, mine], thr.at[2 * s, 0], 10 + 4 * s)
        for p in range(2):
            cols = pl.ds(pl.multiple_of(units(s, 1 - p) * BLK, BLK), BLK)
            tload[2 * s + 1, p] = load(vthr.at[s, mine, cols], thr.at[2 * s + 1, p], 11 + 4 * s + p)
    small = [
        pltpu.make_async_copy(src, dst, lsem.at[17 + i])
        for i, (src, dst) in enumerate(((vbias_in, vbias), (hbias_in, hbias), (temps_in, temps), (phase_in, phase), (accept_in, accept)))
    ]
    for copy in small:
        copy.start()

    barrier = pltpu.get_barrier_semaphore()
    peers = [(t, col(1)), (t, col(-1)), (t, col(2)), (rep(1), m), (rep(-1), m)]
    peers += [(temp_of(1, 0), m), (temp_of(-1, 0), m), (temp_of(0, 1), m), (temp_of(0, -1), m)]
    for peer in peers:
        pl.semaphore_signal(barrier, inc=1, device_id=peer, device_id_type=MESH)
    pl.semaphore_wait(barrier, len(peers))

    for copy in small:
        copy.wait()
    beta = temps[0]
    meta[...] = jnp.full((8, 128), beta, F32)
    meta[0:2, :] = accept[...].astype(F32)

    sibling = (t + 1 - 2 * c, m)

    def place(name, seen):
        p = name[0]
        _, hop, (oy, oz), first, rows, _ = MSGS[INDEX[name]]
        sy, sz = hop or (0, 0)
        start = temp_of(oy - (sy if seen else 0), oz - (sz if seen else 0)) * 64 + first
        return W.at[p, pl.ds(pl.multiple_of(start, 8), rows)]

    def launch(name):
        i = INDEX[name]
        ref = place(name, False)
        if MSGS[i][1] is None:
            start = pl.multiple_of(temp_of(*MSGS[i][2]) * 64, 64)
            send(W.at[0, pl.ds(start, 64)], ref, gs.at[1], gr.at[SEMS[hop(name)]], far)
            return
        send(ref, ref, gs.at[name[0]], gr.at[SEMS[hop(name)]], (temp_of(*MSGS[i][1]), m))

    def to_sibling(p, ref):
        send(ref, ref, dsem.at[p, 0], dsem.at[p, 1], sibling)

    wload.wait()
    for name in SENDS[None]:
        launch(name)
    send(W.at[0, block], W.at[1, block], xs.at[0], xr.at[0], far)
    to_sibling(0, W.at[0, block])
    own_v = V.at[0, pl.ds(4 * m, 4)]
    for e in (0, 1):
        send(meta, metar.at[e], ms.at[0], ms.at[1], (rep(1 - 2 * e), m))

    def send_chains():
        for cp in vload:
            cp.wait()
        send(own_v, own_v, xs.at[1], xr.at[1], partner)
        for cp in oload:
            cp.wait()
        send(CO, own_v, xs.at[1], xr.at[1], other)
        send(CO, own_v, xs.at[1], xr.at[1], far)
        send(hbias, hbr, xs.at[2], xr.at[2], far)

    def send_thresholds(s):
        tload[2 * s, 1].wait()
        TS[s] = thr[2 * s, 1].astype(F32).astype(BF16)
        send(TS.at[s], TR.at[s], xs.at[3], xr.at[3 + s], far)

    def prepare(k, p):
        if k % 2 == 0 and p == 1:
            arrived(TR.at[k // 2], xr.at[3 + k // 2])
            if k == 0:
                arrived(hbr, xr.at[2])
        else:
            tload[k, p].wait()

        def some(i, carry):
            r = pl.ds(pl.multiple_of(i * 32, 32), 32)
            if k % 2 == 0 and p == 1:
                value, bias = TR[k // 2, r, :], hbr[...]
            else:
                value, bias = thr[k, p, r, :], (hbias[...] if k % 2 == 0 else vbias[units(k // 2, 1 - p)])
            level = (value.astype(F32) + 0.5) / 256.0
            L[k, p, r, :] = beta * bias + (jnp.log(level) - jnp.log(1.0 - level))
            return carry

        lax.fori_loop(0, HALF // 32, some, 0)

    def decisions():
        arrived(metar, ms.at[1])
        low, up = metar.at[0], metar.at[1]
        ph = phase[...]
        lower = (lax.rem(t, 2) == ph) & (t + 1 < NT)
        upper = (lax.rem(t + 1, 2) == ph) & (t >= 1)
        take_up = jnp.where(lower & (accept[...] == 1), 1.0, 0.0)
        take_low = jnp.where(upper & (low[0:2, :] > 0.5), 1.0, 0.0)
        b = jnp.where(take_up > 0.5, up[2:4, :], jnp.where(take_low > 0.5, low[2:4, :], jnp.full((2, 128), beta, F32)))
        for h in (0, 1):
            for ref, rows in ((TU, take_up), (TL, take_low)):
                ref[128 * h : 128 * h + 128, :] = jnp.broadcast_to(rows[h : h + 1, :], (128, 128)).T
        BT[...] = jnp.broadcast_to(jnp.where(a == 0, b[0:1, :], b[1:2, :]), (128, 128)).T
        return take_up, take_low

    def dot(x, w):
        return jnp.dot(x, w, preferred_element_type=F32)

    def dot_t(x, w):
        return lax.dot_general(x, w, (((1,), (1,)), ((), ())), preferred_element_type=F32)

    def wrows(k):
        return pl.ds(pl.multiple_of(k * CW, CW), CW)

    def add_product(ph, p, chunks, fresh, tiles=range(4)):
        for n in tiles:
            cols = pl.ds(n * CW, CW)
            total = None
            for k in chunks:
                part = dot(V[ph, k], W[p, wrows(k), cols])
                total = part if total is None else total + part
            acc[p, :, cols] = total if fresh else acc[p, :, cols] + total

    def hidden_states(s, p):
        def tile(n, carry):
            cols = pl.ds(pl.multiple_of(n * CW, CW), CW)
            H[s, p, :, cols] = jax.nn.sigmoid(beta * acc[p, :, cols] + L[2 * s, p, :, cols]).astype(BF16)
            return carry

        lax.fori_loop(0, 4, tile, 0)

    def first_half():
        half0 = W.at[0, pl.ds(0, NT // 2 * 64)]
        arrived(half0, dsem.at[0, 1])
        arrived(V.at[0, pl.ds(0, 12)], xr.at[1])

    def first_partials(g):
        for k in (2 * g, 2 * g + 1):
            PA[k] = dot_t(H[0, 0], W[0, wrows(k), :])

    flags = None
    early = [send_chains, lambda: send_thresholds(0)]
    early += [lambda k=k, p=p: prepare(k, p) for k, p in ((0, 0), (1, 0), (1, 1), (2, 0), (3, 0), (3, 1))]
    late = [first_half, lambda: send_thresholds(1)] + [lambda n=n: add_product(0, 0, range(16), True, (n,)) for n in range(4)]
    late += [lambda: hidden_states(0, 0)] + [lambda g=g: first_partials(g) for g in range(8)]
    late += [lambda: prepare(0, 1)]
    for n, names in enumerate(WAITS):
        p = names[0][0]
        if names[0][1] == "XW":
            refs = [W.at[1, block]]
            arrived(refs[0], xr.at[0])
        else:
            refs = [place(name, True) for name in names]
            total = sum(MSGS[INDEX[name]][4] for name in names)
            arrived(W.at[p, pl.ds(0, total)], gr.at[SEMS[hop(names[0])]])
        for nxt in SENDS[hop(names[0])]:
            launch(nxt)
        for ref in refs:
            to_sibling(p, ref)
        if n >= START and n % 2 == 0 and early:
            early.pop(0)()
        if n == 18:
            flags = decisions()
        for _ in range(2):
            if n >= LAST0 + 2 and late:
                late.pop(0)()
    for job in early + late:
        job()
    take_up, take_low = flags
    arrived(W.at[1, pl.ds(0, NT // 2 * 64)], dsem.at[1, 1])

    def partial(s, k):
        if s == 0:
            return PA[k] + dot_t(H[0, 1], W[1, wrows(k), :])
        return dot_t(H[s, 0], W[0, wrows(k), :]) + dot_t(H[s, 1], W[1, wrows(k), :])

    def visible_states(s):
        def give(i, term):
            SB[s, i] = term.astype(BF16)
            send(SB.at[s, i], RB.at[s, i], rss.at[s], rsr.at[s, i], partner)

        def keep(i, own):
            j, half = i % 4, i // 4
            k = 4 * units(s, half) + j
            arrived(RB.at[s, i], rsr.at[s, i])
            pre = own + RB[s, i].astype(F32)
            V[s + 1, k] = jax.nn.sigmoid(beta * pre + L[2 * s + 1, 1 - half, :, j * CW : j * CW + CW]).astype(BF16)
            ref = V.at[s + 1, k]
            send(ref, ref, ags.at[s], agr.at[s, i], partner)
            if s < SWEEPS - 1:
                return
            if half == 0:
                send(ref, VX.at[j], fs.at[1], fr.at[1 + j], other)
                return
            swap(ref, lambda e: swapv.at[e, a, j], 1)

        jobs = [(give, i, 4 * units(s, i // 4, True) + i % 4) for i in range(8)]
        jobs += [(keep, i, 4 * units(s, i // 4) + i % 4) for i in range(8)]
        def terms(n):
            return [partial(s, jobs[n + e][2]) for e in (0, 1)]

        ahead = terms(0)
        for n in range(0, len(jobs), 2):
            now, ahead = ahead, (terms(n + 2) if n + 2 < len(jobs) else None)
            for e in (0, 1):
                job, i, _ = jobs[n + e]
                job(i, now[e])
            if s == SWEEPS - 1 and n == HY_AT:
                arrived(HX, fr.at[0])
                swap(HX, lambda e: swaph.at[e, 1 - a], 0)

    def swap(src, dst, kind):
        for e in (0, 1):

            @pl.when(t + 1 < NT if e == 0 else t >= 1)
            def _():
                send(src, dst(e), sws.at[kind, e], swr.at[kind, e], (rep(1 - 2 * e), m))

    def gathered_product(ph):
        own = [4 * units(ph - 1, i // 4) + i % 4 for i in range(8)]
        if ph == SWEEPS:
            swap_far(0)
        add_product(ph, 0, own, True)
        if ph == SWEEPS:
            swap_far(1)
        add_product(ph, 1, own, True)
        if ph == 1:
            prepare(2, 1)
        for i in range(0, 8, 2):
            ks = [4 * units(ph - 1, i // 4, True) + i % 4 + e for e in (0, 1)]
            for e in (0, 1):
                arrived(V.at[ph, ks[e]], agr.at[ph - 1, i + e])
            for p in (0, 1):
                add_product(ph, p, ks, False)
            if ph == SWEEPS and i < 4:
                swap_far(2 + i // 2)

    def swap_far(j):
        arrived(VX.at[j], fr.at[1 + j])
        swap(VX.at[j], lambda e: swapv.at[e, 1 - a, j], 1)

    add_product(0, 1, range(16), True)
    hidden_states(0, 1)
    visible_states(0)
    gathered_product(1)
    hidden_states(1, 1)
    send(H.at[1, 1], HX, fs.at[0], fr.at[0], far)
    hidden_states(1, 0)
    swap(H.at[1, 0], lambda e: swaph.at[e, a], 0)
    visible_states(1)

    def lanes(g):
        return pl.ds(pl.multiple_of(g * 128, 128), 128)

    total = jnp.zeros((HALF, 128), F32)
    for p in (0, 1):
        q = units(SWEEPS - 1, 1 - p)

        def bias_part(g, value):
            return value + V[2, 4 * q + g // 2, :, lanes(lax.rem(g, 2))].astype(F32) * vbias[q, :, lanes(g)]

        total = lax.fori_loop(0, 8, bias_part, total)
    total = BT[...] * total
    gathered_product(2)
    for p in (0, 1):
        bias_ref = hbr if p else hbias

        def soft_part(g, value):
            x = BT[...] * (acc[p, :, lanes(g)] + bias_ref[:, lanes(g)])
            return value + (jnp.maximum(x, 0.0) + jnp.log(1.0 + jnp.exp(-jnp.abs(x))))

        total = lax.fori_loop(0, 8, soft_part, total)
    ebuf[m] = jnp.broadcast_to(jnp.sum(total.T, axis=0, keepdims=True) * (-1.0 / NH), (8, 128))
    targets = [(0, d) for d in (1, 2, 3)] + [(e, d) for e in (1, -1) for d in range(4)]
    for e, d in targets:
        send(ebuf.at[m], ebuf.at[(e % 3) * NX + m], es.at[0], es.at[1], (rep(e), col(d)))

    def swapped(ref, kind):
        for e in (0, 1):
            there = t >= 1 if e == 0 else t + 1 < NT

            @pl.when(there)
            def _():
                arrived(ref.at[e], swr.at[kind, e])

            @pl.when(jnp.logical_not(there))
            def _():
                ref[e] = jnp.zeros(ref.shape[1:], BF16)

    swapped(swaph, 0)

    def chosen(rows, up, low, own):
        value = jnp.where(TL[rows, :] > 0.5, low.astype(F32), own.astype(F32))
        return jnp.where(TU[rows, :] > 0.5, up.astype(F32), value).astype(BF16)

    def swap_hidden(g, carry):
        cols = lanes(g)
        hid_out[mine, cols] = chosen(mine, swaph[1, a, :, cols], swaph[0, a, :, cols], H[1, 0, :, cols])
        hid_out[theirs, cols] = chosen(theirs, swaph[1, 1 - a, :, cols], swaph[0, 1 - a, :, cols], HX[:, cols])
        return carry

    lax.fori_loop(0, 8, swap_hidden, 0)
    swapped(swapv, 1)

    def swap_visible(g, carry):
        k, cols, out = g // 2, lanes(lax.rem(g, 2)), lanes(g)
        vis_out[mine, out] = chosen(mine, swapv[1, a, k, :, cols], swapv[0, a, k, :, cols], V[2, 4 * m + k, :, cols])
        vis_out[theirs, out] = chosen(theirs, swapv[1, 1 - a, k, :, cols], swapv[0, 1 - a, k, :, cols], VX[k, :, cols])
        return carry

    lax.fori_loop(0, 8, swap_visible, 0)
    arrived(ebuf.at[pl.ds(0, 11)], es.at[1])

    def summed(k):
        parity = c if k == 0 else 1 - c
        low = ebuf[k * NX + parity, 0:1, :] + ebuf[k * NX + parity + 1, 0:1, :]
        high = ebuf[k * NX + parity + 2, 0:1, :] + ebuf[k * NX + lax.rem(parity + 3, NX), 0:1, :]
        return low, high

    sums = [summed(k) for k in range(3)]
    for h in (0, 1):
        value = jnp.where(take_low[h : h + 1] > 0.5, sums[1][h], sums[0][h])
        energy_out[h : h + 1, :] = jnp.where(take_up[h : h + 1] > 0.5, sums[2][h], value)

    for p in (0, 1):
        arrived(W.at[p, pl.ds(0, 31 * 64)], gs.at[p])
        arrived(W.at[p, pl.ds(0, NT // 2 * 64)], dsem.at[p, 0])
    arrived(W.at[0, block], xs.at[0])
    arrived(V.at[0, pl.ds(0, 12)], xs.at[1])
    arrived(hbr, xs.at[2])
    arrived(TR, xs.at[3])
    arrived(metar, ms.at[0])
    arrived(HX, fs.at[0])
    arrived(VX, fs.at[1])
    arrived(ebuf.at[pl.ds(0, 11)], es.at[0])
    for s in range(SWEEPS):
        arrived(SB.at[s], rss.at[s])
        arrived(SB.at[s], ags.at[s])
    for e in (0, 1):

        @pl.when(t + 1 < NT if e == 0 else t >= 1)
        def _():
            arrived(swaph.at[e], sws.at[0, e])
            arrived(swapv.at[e], sws.at[1, e])


def hand_out(vis, hid, energy, vis_out, hid_out, energy_out, sem):
    copies = [
        pltpu.make_async_copy(src, dst, sem.at[i])
        for i, (src, dst) in enumerate(((vis, vis_out), (hid, hid_out), (energy, energy_out)))
    ]
    for copy in copies:
        copy.start()
    for copy in copies:
        copy.wait()


def on_device(
    chains, weights, visible_bias, hidden_bias, inv_temps, hidden_thresholds, visible_thresholds, swap_phase, swap_accept
):
    vmem = pl.BlockSpec(memory_space=pltpu.VMEM)
    hbm = pl.BlockSpec(memory_space=pl.ANY)
    dma, mem = pltpu.SemaphoreType.DMA, pltpu.VMEM
    n = len(SEMS)
    vis, hid, energy = pl.pallas_call(
        kernel,
        out_shape=(mem((ROWS, BLK), BF16), mem((ROWS, BLK), BF16), mem((2, 128), F32)),
        in_specs=[hbm] * 9,
        out_specs=(vmem, vmem, vmem),
        scratch_shapes=[
            mem((2, 4096, BLK), BF16),
            mem((3, 16, HALF, CW), BF16),
            mem((4, HALF, CW), BF16),
            mem((4, 2, HALF, BLK), I32),
            mem((2, HALF, BLK), BF16),
            mem((2, HALF, BLK), BF16),
            mem((1, BLK), F32),
            mem((4, 2, HALF, BLK), F32),
            mem((2, HALF, BLK), F32),
            mem((16, HALF, CW), F32),
            mem((2, 2, HALF, BLK), BF16),
            mem((HALF, BLK), BF16),
            mem((4, HALF, CW), BF16),
            mem((2, 8, HALF, CW), BF16),
            mem((2, 8, HALF, CW), BF16),
            mem((8, 128), F32),
            mem((2, 8, 128), F32),
            mem((2, 2, 4, HALF, CW), BF16),
            mem((2, 2, HALF, BLK), BF16),
            mem((HALF, 128), F32),
            mem((ROWS, 128), F32),
            mem((ROWS, 128), F32),
            mem((12, 8, 128), F32),
            mem((4, 1, BLK), F32), mem((1, BLK), F32), pltpu.SMEM((1,), F32), mem((2, 128), I32), mem((2, 128), I32),
            dma((2,)), dma((n,)), dma((2, 2)), dma((4,)), dma((5,)),
            dma((2,)), dma((2, 8)), dma((2,)), dma((2, 8)), dma((2,)), dma((5,)),
            dma((2, 2)), dma((2, 2)), dma((2,)), dma((2,)), dma((22,)),
        ],
        compiler_params=pltpu.CompilerParams(
            collective_id=0, has_side_effects=True, vmem_limit_bytes=58 * 2**20
        ),
        name="tempered",
    )(
        chains,
        weights,
        visible_bias.reshape(4, 1, BLK),
        hidden_bias.reshape(1, BLK),
        inv_temps,
        hidden_thresholds,
        visible_thresholds,
        swap_phase.reshape(2, 128),
        swap_accept.reshape(2, 128),
    )
    vis, hid, energy = pl.pallas_call(
        hand_out,
        out_shape=(
            jax.ShapeDtypeStruct((ROWS, BLK), BF16),
            jax.ShapeDtypeStruct((ROWS, BLK), BF16),
            jax.ShapeDtypeStruct((2, 128), F32),
        ),
        in_specs=[vmem, vmem, vmem],
        out_specs=(hbm, hbm, hbm),
        scratch_shapes=[dma((3,))],
        name="hand_out",
    )(*(pltpu.with_memory_space_constraint(x, pltpu.VMEM) for x in (vis, hid, energy)))
    return vis, hid, energy.reshape(ROWS)


def solution(mesh):
    return jax.shard_map(
        on_device,
        mesh=mesh,
        in_specs=(
            P("temp", "mp"),
            P("temp", "mp"),
            P(),
            P("mp"),
            P("temp"),
            P(None, "temp", "mp"),
            P(None, "temp", None),
            P(),
            P("temp"),
        ),
        out_specs=(P("temp", "mp"), P("temp", "mp"), P("temp")),
        check_vma=False,
    )
```
